128 devices in a mesh: aa: 16 (over x, z_hi, core), ba: 8 (over y, z_lo).
Axes of the slice: x: 4, y: 4, z: 4 (z_hi: 2, z_lo: 2; z = z_hi * 2 + z_lo), core: 2. Of those that a mesh axis runs over, the one named last changes fastest.
Arguments:
- amplitudes: bfloat16 [2048, 2048], P('aa', 'ba'), may hold values from -6 to 6
- code: int32 [32, 2048], replicated, may hold values from -2048 to 2048, as said below
- counts: int32 [128], replicated, may hold values from 1 to 16, as said below
- pair_irrep: int32 [32], replicated, may hold values from 0 to 7
- integrals: bfloat16 [32, 32], replicated, may hold values from -3 to 3
- one_body: bfloat16 [32], replicated, may hold values from -1.5 to 1.5
Outputs:
- sigma: bfloat16 [2048, 2048], P('aa', 'ba')
The draws below stay inside these ranges and needn't reach their ends.
Inputs may be any that keep to these rules, and one draw needn't show every extreme that they name: |code| - 1 names the target string of a replacement and the sign of code its sign; some entries reach both ends. `counts`: the live strings of fine block j fill its first slots, from slot j * 16 on; in every draw some block is full and some holds one string.
All inputs are finite; a program needn't handle non-finite values.
Results may differ from the reference program's by a relative error of at most 0.0045.
Values may be sent and summed in bfloat16 or wider, within the bound.
A program may use at most 128 MiB of HBM per device.

```python
import jax
import jax.numpy as jnp
from jax import lax

CAP = 16
PAIRS = 32
IRREPS = 8
BLOCKS = 128
NS = 2048


def draw_code(key, part):
    keys = jax.random.split(jax.random.fold_in(key, 11), 3)
    keep = jax.random.randint(keys[0], (PAIRS, NS), 0, 2)
    target = jax.random.randint(keys[1], (PAIRS, NS), 0, NS)
    sign = 2 * jax.random.randint(keys[2], (PAIRS, NS), 0, 2) - 1
    code = keep * sign * (target + 1)
    code = code.at[0, 0].set(NS).at[0, 1].set(0 - NS)
    return code.astype(jnp.int32)


def draw_counts(key, part):
    keys = jax.random.split(jax.random.fold_in(key, 23), 3)
    values = jax.random.randint(keys[0], (BLOCKS,), 1, CAP + 1)
    first = jax.random.randint(keys[1], (), 0, BLOCKS)
    step = jax.random.randint(keys[2], (), 1, BLOCKS)
    second = (first + step) % BLOCKS
    values = values.at[first].set(CAP).at[second].set(1)
    return values.astype(jnp.int32)


def place_ends(array, key, least, top_value):
    dims = array.shape
    place = [jax.random.randint(jax.random.fold_in(key, axis), (), 0, dims[axis]) for axis in range(len(dims))]
    array = array.at[tuple(place)].set(least)
    longest = dims.index(max(dims))
    place[longest] = (place[longest] + 1) % dims[longest]
    return array.at[tuple(place)].set(top_value)


def steps_of(own_key, extent, cuts, smallest, high):
    gain = 1.0
    for dim, parts in cuts:
        steps = jax.random.uniform(jax.random.fold_in(jax.random.fold_in(own_key, 6), dim), (parts,), jnp.float32, smallest / len(cuts), high / len(cuts))
        gain = gain * jnp.repeat(jnp.exp(steps), extent[dim] // parts).reshape((-1,) + (1,) * (len(extent) - 1 - dim))
    return gain


def bell_draw(rng, shape, spread, bound, shards=(), held_as=jnp.bfloat16):
    values = jax.random.normal(rng, shape, jnp.float32) * spread
    if len(shards) > 0:
        values = steps_of(rng, shape, shards, -0.22, 0.18) * values
    return jnp.clip(values, min=-bound, max=bound).astype(held_as)


def setup_inputs(seed: int = 0) -> dict:
    key_of = jax.random.split(jax.random.key(seed), 7)
    return {
        "amplitudes": bell_draw(key_of[0], (NS, NS), 1.0, 6.0, ((0, 16), (1, 8))),
        "code": draw_code(jax.random.fold_in(key_of[6], 71), 0),
        "counts": draw_counts(jax.random.fold_in(key_of[6], 71), 0),
        "pair_irrep": place_ends(jax.random.randint(key_of[3], (PAIRS,), 0, IRREPS), jax.random.fold_in(key_of[3], 1), 0, IRREPS - 1).astype(jnp.int32),
        "integrals": bell_draw(key_of[4], (PAIRS, PAIRS), (PAIRS // 8) ** -0.5, 3.0),
        "one_body": bell_draw(key_of[5], (PAIRS,), 0.25, 1.5),
    }


def live_of(counts):
    slots = jnp.arange(NS, dtype=jnp.int32)
    return (slots % CAP < counts[slots // CAP]).astype(jnp.float32)


def reference(amplitudes, code, counts, pair_irrep, integrals, one_body):
    live = live_of(counts)
    masked = (amplitudes.astype(jnp.float32) * (live[:, None] * live[None, :])).astype(jnp.bfloat16)
    masked_wide = masked.astype(jnp.float32)
    target = jnp.maximum(jnp.abs(code) - 1, 0).astype(jnp.int32)
    signs = jnp.sign(code).astype(jnp.float32)
    weights = jnp.where(pair_irrep[:, None] == pair_irrep[None, :], integrals, jnp.zeros((), integrals.dtype))
    order = jnp.arange(PAIRS, dtype=jnp.int32)

    def beta_side(pair):
        return (masked_wide[:, target[pair]] * (signs[pair] * live)[None, :]).astype(jnp.bfloat16)

    def alpha_side(pair):
        return (masked_wide[target[pair], :] * (signs[pair] * live)[:, None]).astype(jnp.bfloat16)

    dbeta = lax.map(beta_side, order)
    dalpha = lax.map(alpha_side, order)
    flat_beta = dbeta.reshape(PAIRS, NS * NS)
    flat_alpha = dalpha.reshape(PAIRS, NS * NS)
    gains = one_body.astype(jnp.float32)

    def accumulate(total, pair):
        row = lax.dynamic_slice_in_dim(weights, pair, 1, 0)
        gbeta_full = jnp.dot(row, flat_beta, preferred_element_type=jnp.float32).reshape(NS, NS)
        galpha_full = jnp.dot(row, flat_alpha, preferred_element_type=jnp.float32).reshape(NS, NS)
        gbeta_wide = gbeta_full.astype(jnp.bfloat16).astype(jnp.float32)
        combined_wide = (gbeta_full + 0.5 * galpha_full).astype(jnp.bfloat16).astype(jnp.float32)
        tgt = target[pair]
        sgn = signs[pair]
        total = total + gains[pair] * (dbeta[pair].astype(jnp.float32) + dalpha[pair].astype(jnp.float32))
        total = total + sgn[None, :] * (0.5 * gbeta_wide[:, tgt])
        total = total + sgn[:, None] * combined_wide[tgt, :]
        return total, None

    total, _ = lax.scan(accumulate, jnp.zeros((NS, NS), jnp.float32), order)
    return (total * (live[:, None] * live[None, :])).astype(jnp.bfloat16)
```

```python
import functools

import jax
import jax.numpy as jnp
from jax import lax
from jax.experimental import pallas as pl
from jax.experimental.pallas import tpu as pltpu
from jax.sharding import PartitionSpec as P

F32 = jnp.float32
BF16 = jnp.bfloat16
MESH = pl.DeviceIdType.MESH


def iota(shape, axis):
    return lax.broadcasted_iota(jnp.int32, shape, axis)


def dot(a, b):
    return jnp.dot(a, b, preferred_element_type=F32)


def dot_nt(a, b):
    return lax.dot_general(a, b, (((1,), (1,)), ((), ())), preferred_element_type=F32)


def kernel(
    na, nb, capacity,
    amp_ref, code_ref, counts_ref, irrep_ref, integrals_ref, one_body_ref,
    out_ref,
    hi_ref, lo_ref, sg_ref, m2_ref, mt_ref, y_ref, z_ref, zt_ref, kron_ref, res_ref,
    mg_ref, tb_ref, ta_ref, rs_ref, rr_ref,
    m_send, m_recv, t_send, t_recv, c_send, c_recv, r_send, r_recv,
):
    ra, rb = amp_ref.shape
    pairs, ns = code_ref.shape
    his = ns // 128
    half = his // 2
    tr = ns // (na * nb)
    keys = his * tr
    ma = lax.axis_index("aa")
    mb = lax.axis_index("ba")

    def peer_a(k):
        return lax.rem(ma + k, na)

    def peer_b(k):
        return lax.rem(mb + k, nb)

    barrier = pltpu.get_barrier_semaphore()
    for k in range(1, na):
        pl.semaphore_signal(barrier, inc=1, device_id=(peer_a(k), mb), device_id_type=MESH)
    for k in range(1, nb):
        pl.semaphore_signal(barrier, inc=1, device_id=(ma, peer_b(k)), device_id_type=MESH)
    pl.semaphore_wait(barrier, na + nb - 2)

    def m_copy(k):
        return pltpu.make_async_remote_copy(
            src_ref=amp_ref, dst_ref=mg_ref.at[mb], send_sem=m_send.at[k], recv_sem=m_recv.at[mb],
            device_id=(ma, peer_b(k)), device_id_type=MESH)

    def m_arrived(k):
        src = peer_b(k)
        return pltpu.make_async_remote_copy(
            src_ref=amp_ref, dst_ref=mg_ref.at[src], send_sem=m_send.at[k], recv_sem=m_recv.at[src],
            device_id=(ma, src), device_id_type=MESH)

    for k in range(1, nb):
        m_copy(k).start()

    code = code_ref[...]
    target = jnp.abs(code) - 1
    hi = lax.shift_right_arithmetic(target, 7)
    lo = target & 127
    sg = jnp.where(code > 0, 1.0, jnp.where(code < 0, -1.0, 0.0)).astype(F32)
    hi_ref[...] = hi.astype(F32)
    lo_ref[...] = lo.astype(F32)
    sg_ref[...] = sg

    blocks = counts_ref.shape[1]
    counts = jnp.broadcast_to(counts_ref[...].astype(F32), (8, blocks)).astype(BF16)
    spread = (iota((blocks, ns), 1) // capacity == iota((blocks, ns), 0)).astype(F32).astype(BF16)
    slots = (iota((8, ns), 1) % capacity).astype(F32)
    live8 = jnp.where(slots < dot(counts, spread), 1.0, 0.0)
    live = live8[0:1]

    irr = jnp.broadcast_to(irrep_ref[...], (pairs, pairs))
    eye = iota((pairs, pairs), 0) == iota((pairs, pairs), 1)
    irr_col = jnp.sum(jnp.where(eye, irr, 0), axis=1, keepdims=True)
    w = jnp.where(irr_col == irr, integrals_ref[...].astype(F32), 0.0).astype(BF16)
    w_t = dot_nt(eye.astype(F32).astype(BF16), w).astype(BF16)

    grow = (iota((pairs * 8, pairs), 0) // 8 == iota((pairs * 8, pairs), 1)).astype(F32).astype(BF16)
    wide = dot_nt(dot(grow, w).astype(BF16), grow)
    same = iota((pairs * 8, pairs * 8), 0) % 8 == iota((pairs * 8, pairs * 8), 1) % 8
    kron_ref[...] = jnp.where(same, wide, 0.0).astype(BF16)

    first = mb * rb + ma * tr
    base = pl.multiple_of((first // 128) * 128, 128)
    off = first - base
    n = pairs * tr
    own = jnp.concatenate(
        [hi_ref[:, pl.ds(base, 128)], lo_ref[:, pl.ds(base, 128)], sg_ref[:, pl.ds(base, 128)]], axis=0
    ).astype(BF16)
    pick = (iota((128, n), 0) == off + iota((128, n), 1) % tr).astype(F32).astype(BF16)
    mine = dot(own, pick)
    here = iota((pairs, n), 0) == iota((pairs, n), 1) // tr
    k_hi = jnp.sum(jnp.where(here, mine[0:pairs], 0.0), axis=0, keepdims=True)
    k_lo = jnp.sum(jnp.where(here, mine[pairs : 2 * pairs], 0.0), axis=0, keepdims=True)
    k_sg = jnp.sum(jnp.where(here, mine[2 * pairs :], 0.0), axis=0, keepdims=True)
    here_b = here.astype(F32).astype(BF16)
    w_wide = dot(w_t, here_b)
    o_wide = dot(jnp.broadcast_to(one_body_ref[...], (8, pairs)), here_b)[0:1]
    k_lo_b = k_lo.astype(BF16)
    iota128 = iota((128, n), 0).astype(F32).astype(BF16)
    one = jnp.ones((), BF16)
    zero = jnp.zeros((), BF16)
    planes = jnp.concatenate([hi_ref[...], lo_ref[...], sg_ref[...] * live], axis=0).astype(BF16)
    got = jnp.zeros((3 * pairs, n), F32)
    for h in range(0, his, 2):
        sel = []
        for e in range(2):
            loc = jnp.where(k_hi == float(h + e), k_lo, -1.0).astype(BF16)
            sel.append(jnp.where(iota128 == loc, one, zero))
        got = got + dot(planes[:, h * 128 : (h + 2) * 128], jnp.concatenate(sel, axis=0))
    row = (iota((pairs, n), 1) % tr).astype(F32)
    key_all = got[0:pairs] * float(tr) + row
    lo_all = got[pairs : 2 * pairs]
    val_all = 0.5 * w_wide * got[2 * pairs :] * k_sg
    iota_keys = iota((keys, n), 0).astype(F32).astype(BF16)

    def histogram(key, low, val):
        a = jnp.where(iota_keys == key.astype(BF16), val.astype(BF16), zero)
        b = jnp.where(iota128 == low.astype(BF16), one, zero)
        return dot_nt(a, b)

    t_acc = histogram(k_hi * float(tr) + row[0:1], k_lo, o_wide * k_sg)
    for q in range(pairs):
        t_acc = t_acc + histogram(key_all[q : q + 1], lo_all[q : q + 1], val_all[q : q + 1])
    tb_ref[ma] = t_acc.astype(BF16).reshape(his, tr, 128)

    def t_copy(k, slot):
        return pltpu.make_async_remote_copy(
            src_ref=tb_ref.at[slot], dst_ref=tb_ref.at[slot], send_sem=t_send.at[k], recv_sem=t_recv.at[slot],
            device_id=(peer_a(k), mb), device_id_type=MESH)

    for k in range(1, na):
        t_copy(k, ma).start()

    low_a = ma * ra
    block_of = (iota((ra, blocks), 0) + low_a) // capacity
    count_a = jnp.sum(
        jnp.where(block_of == iota((ra, blocks), 1), counts_ref[...].astype(F32), 0.0), axis=1, keepdims=True)
    live_a = jnp.where(((iota((ra, 1), 0) + low_a) % capacity).astype(F32) < count_a, 1.0, 0.0)
    mg_ref[mb] = amp_ref[...]
    for k in range(1, nb):
        m_arrived(k).wait_recv()
    for j in range(nb):
        part = mg_ref[j].astype(F32) * live_a * live[:, j * rb : (j + 1) * rb]
        h = (j * rb) // (half * 128)
        at = j * rb - h * half * 128
        m2_ref[h * ra : (h + 1) * ra, at : at + rb] = part.astype(BF16)
    low_b = pl.multiple_of(mb * rb, 128)
    res_ref[...] = live8
    live_b = res_ref[0:1, pl.ds(low_b, rb)]
    mine_f = amp_ref[...].astype(F32) * live_a * live_b
    mt_ref[...] = mine_f.T.astype(BF16)

    iota_b = iota((128, rb), 0).astype(F32).astype(BF16)

    def gather(q, carry):
        hi_q = hi_ref[pl.ds(q, 1), pl.ds(low_b, rb)]
        lo_q = lo_ref[pl.ds(q, 1), pl.ds(low_b, rb)]
        sg_q = sg_ref[pl.ds(q, 1), pl.ds(low_b, rb)]
        upper = hi_q >= float(half)
        hi_in = jnp.where(upper, hi_q - float(half), hi_q)
        hots = []
        for j in range(half):
            loc = jnp.where(hi_in == float(j), lo_q, -1.0).astype(BF16)
            hots.append(jnp.where(iota_b == loc, one, zero))
        got_q = dot(m2_ref[...], jnp.concatenate(hots, axis=0))
        picked = jnp.where(jnp.broadcast_to(upper, (ra, rb)), got_q[ra:], got_q[:ra])
        y_ref[q] = picked * (sg_q * live_b)
        return carry

    lax.fori_loop(0, pairs, gather, 0)

    def mix(g, carry):
        at = pl.multiple_of(g * 8, 8)
        rows = y_ref[:, pl.ds(at, 8), :].reshape(pairs * 8, rb).astype(BF16)
        z_ref[:, pl.ds(at, 8), :] = dot(kron_ref[...], rows).reshape(pairs, 8, rb)
        return carry

    lax.fori_loop(0, ra // 8, mix, 0)

    def flip(p, carry):
        zt_ref[p] = z_ref[p].T.astype(BF16)
        return carry

    lax.fori_loop(0, pairs, flip, 0)

    for k in range(1, na):
        t_copy(k, peer_a(k)).wait_recv()
    ta_ref[mb] = tb_ref[:, ma]

    def c_copy(k):
        return pltpu.make_async_remote_copy(
            src_ref=tb_ref.at[:, ma], dst_ref=ta_ref.at[mb], send_sem=c_send.at[k], recv_sem=c_recv.at[mb],
            device_id=(ma, peer_b(k)), device_id_type=MESH)

    def c_arrived(k):
        src = peer_b(k)
        return pltpu.make_async_remote_copy(
            src_ref=tb_ref.at[:, ma], dst_ref=ta_ref.at[src], send_sem=c_send.at[k], recv_sem=c_recv.at[src],
            device_id=(ma, src), device_id_type=MESH)

    for k in range(1, nb):
        c_copy(k).start()

    res = jnp.zeros((rb, ra), F32)
    for h in range(0, his, 2):
        lhs = jnp.concatenate([tb_ref[:, h].reshape(rb, 128), tb_ref[:, h + 1].reshape(rb, 128)], axis=1)
        part = h // half
        at = (h - part * half) * 128
        res = res + dot_nt(lhs, m2_ref[part * ra : (part + 1) * ra, at : at + 256])
    total_ref = z_ref.at[0]
    total_ref[:, :] = res.T

    for k in range(1, nb):
        c_arrived(k).wait_recv()

    width = 2 * ra
    steps = na // 2
    group = min(pairs, 8)
    rows_t = width // (na * tr) if width >= na * tr else 0

    def r_copy(dest):
        return pltpu.make_async_remote_copy(
            src_ref=rs_ref.at[dest], dst_ref=rr_ref.at[ma], send_sem=r_send.at[dest], recv_sem=r_recv.at[ma],
            device_id=(dest, mb), device_id_type=MESH)

    def scatter(i, carry):
        d = lax.rem(ma // 2 + 1 + i, steps)
        at = pl.multiple_of(d * width, 128)
        acc = dot_nt(mt_ref[...], ta_ref[d].reshape(width, 128))
        for p0 in range(0, pairs, group):
            hots = []
            for p in range(p0, p0 + group):
                hit = hi_ref[p : p + 1, pl.ds(at, width)] == ma.astype(F32)
                loc = jnp.where(hit, lo_ref[p : p + 1, pl.ds(at, width)], -1.0).astype(BF16)
                hots.append(jnp.where(iota_b == loc, sg_ref[p : p + 1, pl.ds(at, width)].astype(BF16), zero))
            lhs = jnp.concatenate([zt_ref[p] for p in range(p0, p0 + group)], axis=1)
            acc = acc + dot(lhs, jnp.concatenate(hots, axis=0))
        for e in range(2):
            dest = 2 * d + e
            rs_ref[dest] = acc[:, e * ra : (e + 1) * ra].astype(BF16)

            @pl.when(dest != ma)
            def _():
                r_copy(dest).start()
        return carry

    lax.fori_loop(0, steps, scatter, 0)

    total = total_ref[...]
    out_t = total.T + rs_ref[ma].astype(F32)
    for k in range(1, na):
        src = peer_a(k)
        pltpu.make_async_remote_copy(
            src_ref=rs_ref.at[src], dst_ref=rr_ref.at[src], send_sem=r_send.at[src], recv_sem=r_recv.at[src],
            device_id=(src, mb), device_id_type=MESH).wait_recv()
        out_t = out_t + rr_ref[src].astype(F32)
    out_ref[...] = (out_t.T * live_a * live_b).astype(BF16)

    for k in range(1, nb):
        m_copy(k).wait_send()
        c_copy(k).wait_send()
    for k in range(1, na):
        t_copy(k, ma).wait_send()
        r_copy(peer_a(k)).wait_send()


def per_device(na, nb, amplitudes, code, counts, pair_irrep, integrals, one_body):
    ra, rb = amplitudes.shape
    pairs, ns = code.shape
    his = ns // 128
    tr = ns // (na * nb)
    dma = pltpu.SemaphoreType.DMA
    vmem = pl.BlockSpec(memory_space=pltpu.VMEM)
    return pl.pallas_call(
        functools.partial(kernel, na, nb, ns // counts.shape[0]),
        out_shape=jax.ShapeDtypeStruct((ra, rb), BF16),
        in_specs=[vmem] * 6,
        out_specs=vmem,
        scratch_shapes=[
            pltpu.VMEM((pairs, ns), F32),
            pltpu.VMEM((pairs, ns), F32),
            pltpu.VMEM((pairs, ns), F32),
            pltpu.VMEM((2 * ra, ns // 2), BF16),
            pltpu.VMEM((rb, ra), BF16),
            pltpu.VMEM((pairs, ra, rb), F32),
            pltpu.VMEM((pairs, ra, rb), F32),
            pltpu.VMEM((pairs, rb, ra), BF16),
            pltpu.VMEM((pairs * 8, pairs * 8), BF16),
            pltpu.VMEM((8, ns), F32),
            pltpu.VMEM((nb, ra, rb), BF16),
            pltpu.VMEM((na, his, tr, 128), BF16),
            pltpu.VMEM((nb, na, tr, 128), BF16),
            pltpu.VMEM((na, rb, ra), BF16),
            pltpu.VMEM((na, rb, ra), BF16),
            dma((nb,)), dma((nb,)), dma((na,)), dma((na,)),
            dma((nb,)), dma((nb,)), dma((na,)), dma((na,)),
        ],
        compiler_params=pltpu.CompilerParams(
            collective_id=0, has_side_effects=True, vmem_limit_bytes=56 * 1024 * 1024),
    )(amplitudes, code, counts.reshape(1, -1), pair_irrep.reshape(1, -1), integrals, one_body.reshape(1, -1))


def solution(mesh):
    placed = (P("aa", "ba"), P(), P(), P(), P(), P())
    body = functools.partial(per_device, mesh.shape["aa"], mesh.shape["ba"])
    return jax.shard_map(body, mesh=mesh, in_specs=placed, out_specs=P("aa", "ba"), check_vma=False)
```

```python
import functools

import jax
import jax.numpy as jnp
from jax import lax
from jax.experimental import pallas as pl
from jax.experimental.pallas import tpu as pltpu
from jax.sharding import PartitionSpec as P

F32 = jnp.float32
BF16 = jnp.bfloat16
MESH = pl.DeviceIdType.MESH
GATHER = 8
MIX = 8
FLIP = 16


def iota(shape, axis):
    return lax.broadcasted_iota(jnp.int32, shape, axis)


def dot(a, b):
    return jnp.dot(a, b, preferred_element_type=F32)


def dot_nt(a, b):
    return lax.dot_general(a, b, (((1,), (1,)), ((), ())), preferred_element_type=F32)


def kernel(
    na, nb, capacity,
    amp_ref, code_ref, counts_ref, irrep_ref, integrals_ref, one_body_ref,
    out_ref,
    hi_ref, lo_ref, sg_ref, m2_ref, mt_ref, y_ref, z_ref, zt_ref, kron_ref, res_ref,
    mg_ref, tb_ref, ta_ref, own_ref, xs_ref, xr_ref, rs_ref, rr_ref,
    m_send, m_recv, t_send, t_recv, f_send, f_recv, c_send, c_recv, x_send, x_recv, r_send, r_recv,
):
    ra, rb = amp_ref.shape
    pairs, ns = code_ref.shape
    his = ns // 128
    half = his // 2
    tr = ns // (na * nb)
    keys = his * tr
    ma = lax.axis_index("aa")
    mb = lax.axis_index("ba")

    nc = na // 2
    chip = ma // 2
    core = lax.rem(ma, 2)
    sibling = chip * 2 + 1 - core

    nx = nc // 2
    ny = nb // 2
    z_hi = lax.rem(chip, 2)
    z_lo = lax.rem(mb, 2)

    def peer_chip(k):
        return lax.rem(chip + k, nc)

    def along_x(k, opposite):
        return lax.rem(chip // 2 + k, nx) * 2 + (1 - z_hi if opposite else z_hi)

    def along_y(k, opposite):
        return lax.rem(mb // 2 + k, ny) * 2 + (1 - z_lo if opposite else z_lo)

    def same_core(c):
        return c * 2 + core

    def peer_b(k):
        return lax.rem(mb + k, nb)

    barrier = pltpu.get_barrier_semaphore()
    for k in range(1, nb):
        pl.semaphore_signal(barrier, inc=1, device_id=(ma, peer_b(k)), device_id_type=MESH)
        pl.semaphore_signal(barrier, inc=1, device_id=(sibling, peer_b(k)), device_id_type=MESH)
    for k in range(1, nc):
        pl.semaphore_signal(barrier, inc=1, device_id=(same_core(peer_chip(k)), mb), device_id_type=MESH)
    pl.semaphore_signal(barrier, inc=1, device_id=(sibling, mb), device_id_type=MESH)
    pl.semaphore_wait(barrier, nc + 2 * (nb - 1))

    def m_copy(k, block, dest):
        return pltpu.make_async_remote_copy(
            src_ref=mg_ref.at[block], dst_ref=mg_ref.at[block], send_sem=m_send.at[k], recv_sem=m_recv.at[block],
            device_id=(ma, dest), device_id_type=MESH)

    def m_first(k):
        return pltpu.make_async_remote_copy(
            src_ref=amp_ref, dst_ref=mg_ref.at[mb], send_sem=m_send.at[k], recv_sem=m_recv.at[mb],
            device_id=(ma, along_y(k, k == 0)), device_id_type=MESH)

    def m_relay(k):
        return m_copy(ny + k, along_y(0, True), along_y(k, False))

    near = [k for k in range(1, ny) if k in (1, ny - 1)]
    far = [k for k in range(1, ny) if k not in near]
    for k in [0] + near + far:
        m_first(k).start()

    code = code_ref[...]
    target = jnp.abs(code) - 1
    hi = lax.shift_right_arithmetic(target, 7)
    lo = target & 127
    sg = jnp.where(code > 0, 1.0, jnp.where(code < 0, -1.0, 0.0)).astype(F32)
    hi_ref[...] = hi.astype(F32)
    lo_ref[...] = lo.astype(F32)
    sg_ref[...] = sg

    blocks = counts_ref.shape[1]
    counts = jnp.broadcast_to(counts_ref[...].astype(F32), (8, blocks)).astype(BF16)
    spread = (iota((blocks, ns), 1) // capacity == iota((blocks, ns), 0)).astype(F32).astype(BF16)
    slots = (iota((8, ns), 1) % capacity).astype(F32)
    live8 = jnp.where(slots < dot(counts, spread), 1.0, 0.0)
    live = live8[0:1]

    irr = jnp.broadcast_to(irrep_ref[...], (pairs, pairs))
    eye = iota((pairs, pairs), 0) == iota((pairs, pairs), 1)
    irr_col = jnp.sum(jnp.where(eye, irr, 0), axis=1, keepdims=True)
    w = jnp.where(irr_col == irr, integrals_ref[...].astype(F32), 0.0).astype(BF16)
    w_t = dot_nt(eye.astype(F32).astype(BF16), w).astype(BF16)

    first = mb * rb + ma * tr
    base = pl.multiple_of((first // 128) * 128, 128)
    off = first - base
    n = pairs * tr
    own = jnp.concatenate(
        [hi_ref[:, pl.ds(base, 128)], lo_ref[:, pl.ds(base, 128)], sg_ref[:, pl.ds(base, 128)]], axis=0
    ).astype(BF16)
    pick = (iota((128, n), 0) == off + iota((128, n), 1) % tr).astype(F32).astype(BF16)
    mine = dot(own, pick)
    here = iota((pairs, n), 0) == iota((pairs, n), 1) // tr
    k_hi = jnp.sum(jnp.where(here, mine[0:pairs], 0.0), axis=0, keepdims=True)
    k_lo = jnp.sum(jnp.where(here, mine[pairs : 2 * pairs], 0.0), axis=0, keepdims=True)
    k_sg = jnp.sum(jnp.where(here, mine[2 * pairs :], 0.0), axis=0, keepdims=True)
    here_b = here.astype(F32).astype(BF16)
    w_wide = dot(w_t, here_b)
    o_wide = dot(jnp.broadcast_to(one_body_ref[...], (8, pairs)), here_b)[0:1]
    k_lo_b = k_lo.astype(BF16)
    iota128 = iota((128, n), 0).astype(F32).astype(BF16)
    one = jnp.ones((), BF16)
    zero = jnp.zeros((), BF16)
    planes = jnp.concatenate([hi_ref[...], lo_ref[...], sg_ref[...] * live], axis=0).astype(BF16)
    got = jnp.zeros((3 * pairs, n), F32)
    for h in range(0, his, 2):
        sel = []
        for e in range(2):
            loc = jnp.where(k_hi == float(h + e), k_lo, -1.0).astype(BF16)
            sel.append(jnp.where(iota128 == loc, one, zero))
        got = got + dot(planes[:, h * 128 : (h + 2) * 128], jnp.concatenate(sel, axis=0))
    row = (iota((pairs, n), 1) % tr).astype(F32)
    key_all = got[0:pairs] * float(tr) + row
    lo_all = got[pairs : 2 * pairs]
    val_all = 0.5 * w_wide * got[2 * pairs :] * k_sg
    iota_keys = iota((keys, n), 0).astype(F32).astype(BF16)

    def histogram(key, low, val):
        a = jnp.where(iota_keys == key.astype(BF16), val.astype(BF16), zero)
        b = jnp.where(iota128 == low.astype(BF16), one, zero)
        return dot_nt(a, b)

    t_acc = histogram(k_hi * float(tr) + row[0:1], k_lo, o_wide * k_sg)
    for q in range(pairs):
        t_acc = t_acc + histogram(key_all[q : q + 1], lo_all[q : q + 1], val_all[q : q + 1])
    tb_ref[ma] = t_acc.astype(BF16).reshape(his, tr, 128)

    def t_copy(k, c, dest):
        slot = same_core(c)
        return pltpu.make_async_remote_copy(
            src_ref=tb_ref.at[slot], dst_ref=tb_ref.at[slot], send_sem=t_send.at[k], recv_sem=t_recv.at[c],
            device_id=(same_core(dest), mb), device_id_type=MESH)

    def t_first(k):
        return t_copy(k, chip, along_x(k, k == 0))

    def t_relay(k):
        return t_copy(nx + k, along_x(0, True), along_x(k, False))

    def f_copy(c):
        slot = same_core(c)
        return pltpu.make_async_remote_copy(
            src_ref=tb_ref.at[slot], dst_ref=tb_ref.at[slot], send_sem=f_send.at[c], recv_sem=f_recv.at[c],
            device_id=(sibling, mb), device_id_type=MESH)

    def f_arrived(c):
        slot = c * 2 + 1 - core
        return pltpu.make_async_remote_copy(
            src_ref=tb_ref.at[slot], dst_ref=tb_ref.at[slot], send_sem=f_send.at[c], recv_sem=f_recv.at[c],
            device_id=(sibling, mb), device_id_type=MESH)

    def pass_on(c):
        for k in range(1, nb):
            for e in range(2):
                pltpu.make_async_remote_copy(
                    src_ref=tb_ref.at[same_core(c), chip * 2 + e], dst_ref=ta_ref.at[mb, core, c],
                    send_sem=c_send.at[k, e], recv_sem=c_recv.at[mb, core],
                    device_id=(chip * 2 + e, peer_b(k)), device_id_type=MESH).start()

    def c_sent(k, e):
        return pltpu.make_async_remote_copy(
            src_ref=ta_ref.at[mb, core], dst_ref=ta_ref.at[mb, core], send_sem=c_send.at[k, e],
            recv_sem=c_recv.at[mb, core], device_id=(chip * 2 + e, peer_b(k)), device_id_type=MESH)

    def c_arrived(k, e):
        src = peer_b(k)
        return pltpu.make_async_remote_copy(
            src_ref=ta_ref.at[src, e], dst_ref=ta_ref.at[src, e], send_sem=c_send.at[k, e],
            recv_sem=c_recv.at[src, e], device_id=(chip * 2 + e, src), device_id_type=MESH)

    def hand_over(c):
        t_copy(0, c, chip).wait_recv()
        f_copy(c).start()
        pass_on(c)

    near_x = [k for k in range(1, nx) if k in (1, nx - 1)]
    far_x = [k for k in range(1, nx) if k not in near_x]
    for k in [0] + near_x + far_x:
        t_first(k).start()
    f_copy(chip).start()
    pass_on(chip)

    m_copy(0, along_y(0, True), mb).wait_recv()
    for k in near + far:
        m_relay(k).start()

    grow = (iota((pairs * 8, pairs), 0) // 8 == iota((pairs * 8, pairs), 1)).astype(F32).astype(BF16)
    wide = dot_nt(dot(grow, w).astype(BF16), grow)
    same = iota((pairs * 8, pairs * 8), 0) % 8 == iota((pairs * 8, pairs * 8), 1) % 8
    kron_ref[...] = jnp.where(same, wide, 0.0).astype(BF16)

    low_a = ma * ra
    block_of = (iota((ra, blocks), 0) + low_a) // capacity
    count_a = jnp.sum(
        jnp.where(block_of == iota((ra, blocks), 1), counts_ref[...].astype(F32), 0.0), axis=1, keepdims=True)
    live_a = jnp.where(((iota((ra, 1), 0) + low_a) % capacity).astype(F32) < count_a, 1.0, 0.0)
    mg_ref[mb] = amp_ref[...]
    t_copy(0, along_x(0, True), chip).wait_recv()
    for k in near_x + far_x:
        t_relay(k).start()
    f_copy(along_x(0, True)).start()
    pass_on(along_x(0, True))
    for k in range(1, ny):
        m_copy(0, along_y(k, False), mb).wait_recv()
        m_copy(0, along_y(k, True), mb).wait_recv()
    for j in range(nb):
        part = mg_ref[j].astype(F32) * live_a * live[:, j * rb : (j + 1) * rb]
        h = (j * rb) // (half * 128)
        at = j * rb - h * half * 128
        m2_ref[h * ra : (h + 1) * ra, at : at + rb] = part.astype(BF16)
    low_b = pl.multiple_of(mb * rb, 128)
    res_ref[...] = live8
    live_b = res_ref[0:1, pl.ds(low_b, rb)]
    mine_f = amp_ref[...].astype(F32) * live_a * live_b
    mt_ref[...] = mine_f.T.astype(BF16)

    iota_b = iota((128, rb), 0).astype(F32).astype(BF16)

    def gather_one(q):
        hi_q = hi_ref[pl.ds(q, 1), pl.ds(low_b, rb)]
        lo_q = lo_ref[pl.ds(q, 1), pl.ds(low_b, rb)]
        sg_q = sg_ref[pl.ds(q, 1), pl.ds(low_b, rb)]
        upper = hi_q >= float(half)
        hi_in = jnp.where(upper, hi_q - float(half), hi_q)
        hots = []
        for j in range(half):
            loc = jnp.where(hi_in == float(j), lo_q, -1.0).astype(BF16)
            hots.append(jnp.where(iota_b == loc, one, zero))
        got_q = dot(m2_ref[...], jnp.concatenate(hots, axis=0))
        picked = jnp.where(jnp.broadcast_to(upper, (ra, rb)), got_q[ra:], got_q[:ra])
        y_ref[q] = picked * (sg_q * live_b)

    def gather(i, carry):
        for e in range(GATHER):
            gather_one(i * GATHER + e)
        for at, chunks in enumerate(later):
            @pl.when(i == min(at + 1, trips - 1))
            def _():
                for k, opposite in chunks:
                    hand_over(along_x(k, opposite))
        return carry

    trips = pairs // GATHER
    later = (
        [(k, False) for k in near_x],
        [(k, False) for k in far_x] + [(k, True) for k in near_x],
        [(k, True) for k in far_x],
    )

    lax.fori_loop(0, pairs // GATHER, gather, 0)

    def mix(i, carry):
        for e in range(MIX):
            at = pl.multiple_of((i * MIX + e) * 8, 8)
            rows = y_ref[:, pl.ds(at, 8), :].reshape(pairs * 8, rb).astype(BF16)
            z_ref[:, pl.ds(at, 8), :] = dot(kron_ref[...], rows).reshape(pairs, 8, rb)
        return carry

    lax.fori_loop(0, ra // 8 // MIX, mix, 0)

    def flip(i, carry):
        for e in range(FLIP):
            p = i * FLIP + e
            zt_ref[p] = z_ref[p].astype(BF16).T
        return carry

    lax.fori_loop(0, pairs // FLIP, flip, 0)

    for c in range(nc):
        f_arrived(c).wait_recv()
    for e in range(2):
        for c in range(nc):
            ta_ref[mb, e, c] = tb_ref[c * 2 + e, ma]

    res = jnp.zeros((rb, ra), F32)
    for h in range(0, his, 2):
        lhs = jnp.concatenate([tb_ref[:, h].reshape(rb, 128), tb_ref[:, h + 1].reshape(rb, 128)], axis=1)
        part = h // half
        at = (h - part * half) * 128
        res = res + dot_nt(lhs, m2_ref[part * ra : (part + 1) * ra, at : at + 256])
    total_ref = z_ref.at[0]
    total_ref[:, :] = res.T

    for k in range(1, nb):
        for e in range(2):
            c_arrived(k, e).wait_recv()

    width = 2 * ra
    group = min(pairs, 8)

    def x_copy(c):
        return pltpu.make_async_remote_copy(
            src_ref=xs_ref.at[c], dst_ref=xr_ref.at[c], send_sem=x_send.at[c], recv_sem=x_recv.at[c],
            device_id=(sibling, mb), device_id_type=MESH)

    def r_copy(c):
        return pltpu.make_async_remote_copy(
            src_ref=rs_ref.at[c], dst_ref=rr_ref.at[chip], send_sem=r_send.at[c], recv_sem=r_recv.at[chip],
            device_id=(same_core(c), mb), device_id_type=MESH)

    def r_arrived(c):
        return pltpu.make_async_remote_copy(
            src_ref=rs_ref.at[c], dst_ref=rr_ref.at[c], send_sem=r_send.at[c], recv_sem=r_recv.at[c],
            device_id=(same_core(c), mb), device_id_type=MESH)

    def scatter(i, carry):
        d = peer_chip(1 + i)
        at = pl.multiple_of(d * width, 128)
        columns = jnp.concatenate([ta_ref[d, e, c] for c in range(nc) for e in range(2)], axis=0)
        acc = dot_nt(mt_ref[...], columns)
        for p0 in range(0, pairs, group):
            hots = []
            for p in range(p0, p0 + group):
                hit = hi_ref[p : p + 1, pl.ds(at, width)] == ma.astype(F32)
                loc = jnp.where(hit, lo_ref[p : p + 1, pl.ds(at, width)], -1.0).astype(BF16)
                hots.append(jnp.where(iota_b == loc, sg_ref[p : p + 1, pl.ds(at, width)].astype(BF16), zero))
            lhs = jnp.concatenate([zt_ref[p] for p in range(p0, p0 + group)], axis=1)
            acc = acc + dot(lhs, jnp.concatenate(hots, axis=0))
        first_core = core == 0
        own_ref[d] = jnp.where(first_core, acc[:, :ra], acc[:, ra:])
        xs_ref[d] = jnp.where(first_core, acc[:, ra:], acc[:, :ra])
        x_copy(d).start()

        @pl.when(i > 0)
        def _():
            send(peer_chip(i))
        return carry

    def send(d):
        x_copy(d).wait_recv()
        rs_ref[d] = (own_ref[d] + xr_ref[d]).astype(BF16)
        r_copy(d).start()

    lax.fori_loop(0, nc, scatter, 0)

    x_copy(chip).wait_recv()
    out_t = total_ref[...].T + own_ref[chip] + xr_ref[chip]
    for k in range(1, nc):
        c = peer_chip(nc - k)
        r_arrived(c).wait_recv()
        out_t = out_t + rr_ref[c].astype(F32)
    out_ref[...] = (out_t.T * live_a * live_b).astype(BF16)

    for k in range(ny):
        m_first(k).wait_send()
    for k in range(1, ny):
        m_relay(k).wait_send()
    for k in range(nx):
        t_first(k).wait_send()
    for k in range(1, nx):
        t_relay(k).wait_send()
    for k in range(1, nb):
        for e in range(2):
            c_sent(k, e).wait_send()
    for c in range(nc):
        f_copy(c).wait_send()
        x_copy(c).wait_send()
    for k in range(1, nc):
        r_copy(peer_chip(k)).wait_send()


def per_device(na, nb, amplitudes, code, counts, pair_irrep, integrals, one_body):
    ra, rb = amplitudes.shape
    pairs, ns = code.shape
    his = ns // 128
    tr = ns // (na * nb)
    dma = pltpu.SemaphoreType.DMA
    vmem = pl.BlockSpec(memory_space=pltpu.VMEM)
    return pl.pallas_call(
        functools.partial(kernel, na, nb, ns // counts.shape[0]),
        out_shape=jax.ShapeDtypeStruct((ra, rb), BF16),
        in_specs=[vmem] * 6,
        out_specs=vmem,
        scratch_shapes=[
            pltpu.VMEM((pairs, ns), F32),
            pltpu.VMEM((pairs, ns), F32),
            pltpu.VMEM((pairs, ns), F32),
            pltpu.VMEM((2 * ra, ns // 2), BF16),
            pltpu.VMEM((rb, ra), BF16),
            pltpu.VMEM((pairs, ra, rb), F32),
            pltpu.VMEM((pairs, ra, rb), F32),
            pltpu.VMEM((pairs, rb, ra), BF16),
            pltpu.VMEM((pairs * 8, pairs * 8), BF16),
            pltpu.VMEM((8, ns), F32),
            pltpu.VMEM((nb, ra, rb), BF16),
            pltpu.VMEM((na, his, tr, 128), BF16),
            pltpu.VMEM((nb, 2, na // 2, tr, 128), BF16),
            pltpu.VMEM((na // 2, rb, ra), F32),
            pltpu.VMEM((na // 2, rb, ra), F32),
            pltpu.VMEM((na // 2, rb, ra), F32),
            pltpu.VMEM((na // 2, rb, ra), BF16),
            pltpu.VMEM((na // 2, rb, ra), BF16),
            dma((nb,)), dma((nb,)), dma((na // 2,)), dma((na // 2,)), dma((na // 2,)), dma((na // 2,)),
            dma((nb, 2)), dma((nb, 2)), dma((na // 2,)), dma((na // 2,)), dma((na // 2,)), dma((na // 2,)),
        ],
        compiler_params=pltpu.CompilerParams(
            collective_id=0, has_side_effects=True, vmem_limit_bytes=56 * 1024 * 1024),
    )(amplitudes, code, counts.reshape(1, -1), pair_irrep.reshape(1, -1), integrals, one_body.reshape(1, -1))


def solution(mesh):
    placed = (P("aa", "ba"), P(), P(), P(), P(), P())
    body = functools.partial(per_device, mesh.shape["aa"], mesh.shape["ba"])
    return jax.shard_map(body, mesh=mesh, in_specs=placed, out_specs=P("aa", "ba"), check_vma=False)
```

```python
import functools

import jax
import jax.numpy as jnp
from jax import lax
from jax.experimental import pallas as pl
from jax.experimental.pallas import tpu as pltpu
from jax.sharding import PartitionSpec as P

F32 = jnp.float32
BF16 = jnp.bfloat16
MESH = pl.DeviceIdType.MESH
GATHER = 8
MIX = 8
FLIP = 16


def iota(shape, axis):
    return lax.broadcasted_iota(jnp.int32, shape, axis)


def dot(a, b):
    return jnp.dot(a, b, preferred_element_type=F32)


def dot_nt(a, b):
    return lax.dot_general(a, b, (((1,), (1,)), ((), ())), preferred_element_type=F32)


def kernel(
    na, nb, capacity,
    amp_ref, code_ref, counts_ref, irrep_ref, integrals_ref, one_body_ref,
    out_ref,
    hi_ref, lo_ref, sg_ref, kk_ref, m2_ref, mt_ref, y_ref, z_ref, zt_ref, kron_ref, live_ref,
    mg_ref, tb_ref, ta_ref, own_ref, xs_ref, xr_ref, rs_ref, rr_ref,
    m_send, m_recv, t_send, t_recv, f_send, f_recv, g_send, g_recv, c_send, c_recv, x_send, x_recv, r_send, r_recv,
):
    ra, rb = amp_ref.shape
    pairs, ns = code_ref.shape
    his = ns // 128
    half = his // 2
    tr = ns // (na * nb)
    keys = his * tr
    ma = lax.axis_index("aa")
    mb = lax.axis_index("ba")

    nc = na // 2
    chip = ma // 2
    core = lax.rem(ma, 2)
    sibling = chip * 2 + 1 - core

    nx = nc // 2
    ny = nb // 2
    z_hi = lax.rem(chip, 2)
    z_lo = lax.rem(mb, 2)

    def peer_chip(k):
        return lax.rem(chip + k, nc)

    def along_x(k, opposite):
        return lax.rem(chip // 2 + k, nx) * 2 + (1 - z_hi if opposite else z_hi)

    def along_y(k, opposite):
        return lax.rem(mb // 2 + k, ny) * 2 + (1 - z_lo if opposite else z_lo)

    def same_core(c):
        return c * 2 + core

    def peer_b(k):
        return lax.rem(mb + k, nb)

    barrier = pltpu.get_barrier_semaphore()
    for k in range(1, nb):
        pl.semaphore_signal(barrier, inc=1, device_id=(ma, peer_b(k)), device_id_type=MESH)
        pl.semaphore_signal(barrier, inc=1, device_id=(sibling, peer_b(k)), device_id_type=MESH)
    for k in range(1, nc):
        pl.semaphore_signal(barrier, inc=1, device_id=(same_core(peer_chip(k)), mb), device_id_type=MESH)
    pl.semaphore_signal(barrier, inc=1, device_id=(sibling, mb), device_id_type=MESH)
    pl.semaphore_wait(barrier, nc + 2 * (nb - 1))

    def m_copy(k, block, dest):
        return pltpu.make_async_remote_copy(
            src_ref=mg_ref.at[block], dst_ref=mg_ref.at[block], send_sem=m_send.at[k], recv_sem=m_recv.at[block],
            device_id=(ma, dest), device_id_type=MESH)

    def m_first(k):
        return pltpu.make_async_remote_copy(
            src_ref=amp_ref, dst_ref=mg_ref.at[mb], send_sem=m_send.at[k], recv_sem=m_recv.at[mb],
            device_id=(ma, along_y(k, k == 0)), device_id_type=MESH)

    def m_relay(k):
        return m_copy(ny + k, along_y(0, True), along_y(k, False))

    near = [k for k in range(1, ny) if k in (1, ny - 1)]
    far = [k for k in range(1, ny) if k not in near]
    for k in [0] + near + far:
        m_first(k).start()

    code = code_ref[...]
    target = jnp.abs(code) - 1
    hi = lax.shift_right_arithmetic(target, 7)
    lo = target & 127
    sg = jnp.where(code > 0, 1.0, jnp.where(code < 0, -1.0, 0.0)).astype(F32)
    hi_ref[...] = hi.astype(F32)
    lo_ref[...] = lo.astype(F32)
    sg_ref[...] = sg

    blocks = counts_ref.shape[1]
    counts = jnp.broadcast_to(counts_ref[...].astype(F32), (8, blocks)).astype(BF16)
    spread = (iota((blocks, ns), 1) // capacity == iota((blocks, ns), 0)).astype(F32).astype(BF16)
    slots = (iota((8, ns), 1) % capacity).astype(F32)
    live8 = jnp.where(slots < dot(counts, spread), 1.0, 0.0)
    live = live8[0:1]
    live_ref[...] = live8

    irr = jnp.broadcast_to(irrep_ref[...], (pairs, pairs))
    eye = iota((pairs, pairs), 0) == iota((pairs, pairs), 1)
    irr_col = jnp.sum(jnp.where(eye, irr, 0), axis=1, keepdims=True)
    w = jnp.where(irr_col == irr, integrals_ref[...].astype(F32), 0.0).astype(BF16)
    w_t = dot_nt(eye.astype(F32).astype(BF16), w).astype(BF16)

    first = mb * rb + ma * tr
    base = pl.multiple_of((first // 128) * 128, 128)
    off = first - base
    n = pairs * tr
    own = jnp.concatenate(
        [hi_ref[:, pl.ds(base, 128)], lo_ref[:, pl.ds(base, 128)], sg_ref[:, pl.ds(base, 128)]], axis=0
    ).astype(BF16)
    pick = (iota((128, n), 0) == off + iota((128, n), 1) % tr).astype(F32).astype(BF16)
    mine = dot(own, pick)
    here = iota((pairs, n), 0) == iota((pairs, n), 1) // tr
    k_hi = jnp.sum(jnp.where(here, mine[0:pairs], 0.0), axis=0, keepdims=True)
    k_lo = jnp.sum(jnp.where(here, mine[pairs : 2 * pairs], 0.0), axis=0, keepdims=True)
    k_sg = jnp.sum(jnp.where(here, mine[2 * pairs :], 0.0), axis=0, keepdims=True)
    here_b = here.astype(F32).astype(BF16)
    w_wide = dot(w_t, here_b)
    o_wide = dot(jnp.broadcast_to(one_body_ref[...], (8, pairs)), here_b)[0:1]
    k_lo_b = k_lo.astype(BF16)
    iota128 = iota((128, n), 0).astype(F32).astype(BF16)
    one = jnp.ones((), BF16)
    zero = jnp.zeros((), BF16)
    planes = jnp.concatenate([hi_ref[...], lo_ref[...], sg_ref[...] * live], axis=0).astype(BF16)
    got = jnp.zeros((3 * pairs, n), F32)
    for h in range(0, his, 2):
        sel = []
        for e in range(2):
            loc = jnp.where(k_hi == float(h + e), k_lo, -1.0).astype(BF16)
            sel.append(jnp.where(iota128 == loc, one, zero))
        got = got + dot(planes[:, h * 128 : (h + 2) * 128], jnp.concatenate(sel, axis=0))
    row = (iota((pairs, n), 1) % tr).astype(F32)
    key_all = got[0:pairs] * float(tr) + row
    lo_all = got[pairs : 2 * pairs]
    val_all = 0.5 * w_wide * got[2 * pairs :] * k_sg
    iota_keys = iota((keys, n), 0).astype(F32).astype(BF16)

    def histogram(key, low, val):
        a = jnp.where(iota_keys == key.astype(BF16), val.astype(BF16), zero)
        b = jnp.where(iota128 == low.astype(BF16), one, zero)
        return dot_nt(a, b)

    t_acc = histogram(k_hi * float(tr) + row[0:1], k_lo, o_wide * k_sg)
    for q in range(pairs):
        t_acc = t_acc + histogram(key_all[q : q + 1], lo_all[q : q + 1], val_all[q : q + 1])
    tb_ref[ma] = t_acc.astype(BF16).reshape(his, tr, 128)

    def t_copy(k, c, dest):
        slot = same_core(c)
        return pltpu.make_async_remote_copy(
            src_ref=tb_ref.at[slot], dst_ref=tb_ref.at[slot], send_sem=t_send.at[k], recv_sem=t_recv.at[c],
            device_id=(same_core(dest), mb), device_id_type=MESH)

    def t_first(k):
        return t_copy(k, chip, along_x(k, k == 0))

    def t_relay(k):
        return t_copy(nx + k, along_x(0, True), along_x(k, False))

    def f_copy(c):
        slot = same_core(c)
        return pltpu.make_async_remote_copy(
            src_ref=tb_ref.at[slot], dst_ref=tb_ref.at[slot], send_sem=f_send.at[c], recv_sem=f_recv.at[c],
            device_id=(sibling, mb), device_id_type=MESH)

    def f_arrived(c):
        slot = c * 2 + 1 - core
        return pltpu.make_async_remote_copy(
            src_ref=tb_ref.at[slot], dst_ref=tb_ref.at[slot], send_sem=f_send.at[c], recv_sem=f_recv.at[c],
            device_id=(sibling, mb), device_id_type=MESH)

    hc = nc // 2

    def pass_on(c):
        for k in range(1, nb):
            pltpu.make_async_remote_copy(
                src_ref=tb_ref.at[same_core(c), pl.ds(chip * 2, 2)], dst_ref=ta_ref.at[mb, core, lax.rem(c, hc)],
                send_sem=c_send.at[k, c // hc], recv_sem=c_recv.at[mb, core],
                device_id=(chip * 2 + c // hc, peer_b(k)), device_id_type=MESH).start()

    def c_copy(k, src, e):
        return pltpu.make_async_remote_copy(
            src_ref=ta_ref.at[src, e], dst_ref=ta_ref.at[src, e], send_sem=c_send.at[k, e],
            recv_sem=c_recv.at[src, e], device_id=(chip * 2 + e, peer_b(k)), device_id_type=MESH)

    def hand_over(c):
        t_copy(0, c, chip).wait_recv()
        f_copy(c).start()
        pass_on(c)

    near_x = [k for k in range(1, nx) if k in (1, nx - 1)]
    far_x = [k for k in range(1, nx) if k not in near_x]
    for k in [0] + near_x + far_x:
        t_first(k).start()
    f_copy(chip).start()
    pass_on(chip)

    m_copy(0, along_y(0, True), mb).wait_recv()
    for k in near + far:
        m_relay(k).start()

    grow = (iota((pairs * 8, pairs), 0) // 8 == iota((pairs * 8, pairs), 1)).astype(F32).astype(BF16)
    wide = dot_nt(dot(grow, w).astype(BF16), grow)
    same = iota((pairs * 8, pairs * 8), 0) % 8 == iota((pairs * 8, pairs * 8), 1) % 8
    kron_ref[...] = jnp.where(same, wide, 0.0).astype(BF16)

    low_a = ma * ra
    block_of = (iota((ra, blocks), 0) + low_a) // capacity
    count_a = jnp.sum(
        jnp.where(block_of == iota((ra, blocks), 1), counts_ref[...].astype(F32), 0.0), axis=1, keepdims=True)
    live_a = jnp.where(((iota((ra, 1), 0) + low_a) % capacity).astype(F32) < count_a, 1.0, 0.0)
    mg_ref[mb] = amp_ref[...]
    low_b = pl.multiple_of(mb * rb, 128)
    live_b = live_ref[0:1, pl.ds(low_b, rb)]
    mine_f = amp_ref[...].astype(F32) * live_a * live_b
    mt_ref[core] = mine_f.T.astype(BF16)
    g_copy = pltpu.make_async_remote_copy(
        src_ref=mt_ref.at[core], dst_ref=mt_ref.at[core], send_sem=g_send, recv_sem=g_recv,
        device_id=(sibling, mb), device_id_type=MESH)
    g_copy.start()

    hi_b = hi_ref[:, pl.ds(low_b, rb)]
    y_b = jnp.floor(hi_b * 0.25)
    rest_b = hi_b - 4.0 * y_b
    for turn in range(2):
        e_b = rest_b - 2.0 * (1 - z_lo if turn else z_lo).astype(F32)
        inside = (e_b >= 0.0) & (e_b < 2.0)
        kk_ref[turn] = jnp.where(inside, 2.0 * y_b + e_b, -1.0)

    iota_b = iota((128, rb), 0).astype(F32).astype(BF16)

    def arrange(turn):
        for y in range(ny):
            block = 2 * y + (1 - z_lo if turn else z_lo)
            on = live_ref[0:1, pl.ds(pl.multiple_of(block * rb, 128), rb)]
            part = (mg_ref[block].astype(F32) * live_a * on).astype(BF16)
            for e in range(2):
                u = 2 * y + e
                h, at = u // ny, (u % ny) * 128
                m2_ref[turn, h * ra : (h + 1) * ra, at : at + 128] = part[:, e * 128 : (e + 1) * 128]

    def gather_one(turn, q):
        kk_q = kk_ref[turn, pl.ds(q, 1), :]
        lo_q = lo_ref[pl.ds(q, 1), pl.ds(low_b, rb)]
        sg_q = sg_ref[pl.ds(q, 1), pl.ds(low_b, rb)]
        upper = kk_q >= float(ny)
        inner = jnp.where(upper, kk_q - float(ny), kk_q)
        hots = []
        for j in range(ny):
            loc = jnp.where(inner == float(j), lo_q, -1.0).astype(BF16)
            hots.append(jnp.where(iota_b == loc, one, zero))
        got_q = dot(m2_ref[turn], jnp.concatenate(hots, axis=0))
        picked = jnp.where(jnp.broadcast_to(upper, (ra, rb)), got_q[ra:], got_q[:ra]) * (sg_q * live_b)
        y_ref[q] = y_ref[q] + picked if turn else picked

    trips = pairs // GATHER

    for k in range(1, ny):
        m_copy(0, along_y(k, False), mb).wait_recv()
    arrange(0)

    def gather_own(i, carry):
        for e in range(GATHER):
            gather_one(0, i * GATHER + e)

        @pl.when(i == trips - 2)
        def _():
            t_copy(0, along_x(0, True), chip).wait_recv()
            for k in near_x + far_x:
                t_relay(k).start()
            f_copy(along_x(0, True)).start()
            pass_on(along_x(0, True))
        return carry

    lax.fori_loop(0, trips, gather_own, 0)
    for k in near_x + far_x:
        hand_over(along_x(k, False))
    for k in range(1, ny):
        m_copy(0, along_y(k, True), mb).wait_recv()
    arrange(1)

    def gather_other(i, carry):
        for e in range(GATHER):
            gather_one(1, i * GATHER + e)

        return carry

    lax.fori_loop(0, trips, gather_other, 0)
    for k in near_x:
        hand_over(along_x(k, True))

    def mix(i, carry):
        for e in range(MIX):
            at = pl.multiple_of((i * MIX + e) * 8, 8)
            rows = y_ref[:, pl.ds(at, 8), :].reshape(pairs * 8, rb).astype(BF16)
            z_ref[:, pl.ds(at, 8), :] = dot(kron_ref[...], rows).reshape(pairs, 8, rb)
        return carry

    lax.fori_loop(0, ra // 8 // MIX, mix, 0)
    for k in far_x:
        hand_over(along_x(k, True))

    def flip(i, carry):
        for e in range(FLIP):
            p = i * FLIP + e
            zt_ref[p] = z_ref[p].astype(BF16).T
        return carry

    lax.fori_loop(0, pairs // FLIP, flip, 0)

    for c in range(nc):
        f_arrived(c).wait_recv()
    for e in range(2):
        for c in range(hc):
            ta_ref[mb, e, c] = tb_ref[core * nc + 2 * c + e, pl.ds(chip * 2, 2)]

    res = jnp.zeros((rb, ra), F32)
    for turn in range(2):
        for u in range(0, 2 * ny, min(ny, 2)):
            parts = []
            for v in range(u, u + min(ny, 2)):
                h = 4 * (v // 2) + 2 * (1 - z_lo if turn else z_lo) + v % 2
                parts.append(tb_ref[:, h].reshape(rb, 128))
            h, at = u // ny, (u % ny) * 128
            res = res + dot_nt(
                jnp.concatenate(parts, axis=1), m2_ref[turn, h * ra : (h + 1) * ra, at : at + 128 * len(parts)])
    total_ref = z_ref.at[0]
    total_ref[:, :] = res.T
    g_copy.wait()

    width = 2 * ra
    group = min(pairs, 8)

    def x_copy(c):
        return pltpu.make_async_remote_copy(
            src_ref=xs_ref.at[c], dst_ref=xr_ref.at[c], send_sem=x_send.at[c], recv_sem=x_recv.at[c],
            device_id=(sibling, mb), device_id_type=MESH)

    def r_copy(c):
        return pltpu.make_async_remote_copy(
            src_ref=rs_ref.at[c], dst_ref=rr_ref.at[chip], send_sem=r_send.at[c], recv_sem=r_recv.at[chip],
            device_id=(same_core(c), mb), device_id_type=MESH)

    def r_arrived(c):
        return pltpu.make_async_remote_copy(
            src_ref=rs_ref.at[c], dst_ref=rr_ref.at[c], send_sem=r_send.at[c], recv_sem=r_recv.at[c],
            device_id=(same_core(c), mb), device_id_type=MESH)

    def scatter(i, carry):
        d = turn_of(i)
        at = pl.multiple_of(d * width, 128)
        acc = jnp.zeros((rb, width), F32)
        for p0 in range(0, pairs, group):
            hots = []
            for p in range(p0, p0 + group):
                hit = hi_ref[p : p + 1, pl.ds(at, width)] == ma.astype(F32)
                loc = jnp.where(hit, lo_ref[p : p + 1, pl.ds(at, width)], -1.0).astype(BF16)
                hots.append(jnp.where(iota_b == loc, sg_ref[p : p + 1, pl.ds(at, width)].astype(BF16), zero))
            lhs = jnp.concatenate([zt_ref[p] for p in range(p0, p0 + group)], axis=1)
            acc = acc + dot(lhs, jnp.concatenate(hots, axis=0))
        first_core = core == 0
        own_ref[d] = jnp.where(first_core, acc[:, :ra], acc[:, ra:])
        xs_ref[d] = jnp.where(first_core, acc[:, ra:], acc[:, :ra])
        x_copy(d).start()

        @pl.when(i > 0)
        def _():
            send(turn_of(i - 1))
        return carry

    def turn_of(i):
        return lax.rem(chip // 2 + nx - 1 - lax.rem(i, nx), nx) * 2 + jnp.where(i < nx, 1 - z_hi, z_hi)

    def arrival(i):
        return lax.rem(chip // 2 + 1 + i % nx, nx) * 2 + (1 - z_hi if i < nx else z_hi)

    def summed(d):
        @pl.when(d != mb)
        def _():
            for e in range(2):
                c_copy(1, d, e).wait_recv()
        x_copy(d).wait_recv()
        acc = own_ref[d] + xr_ref[d]
        for h in range(2):
            rows = jnp.concatenate([ta_ref[d, e, c, h] for c in range(hc) for e in range(2)], axis=0)
            acc = acc + dot_nt(mt_ref[h], rows)
        return acc

    def send(d):
        rs_ref[d] = summed(d).astype(BF16)
        r_copy(d).start()

    lax.fori_loop(0, nc, scatter, 0)

    out_t = total_ref[...].T + summed(chip)
    for i in range(nc - 1):
        c = arrival(i)
        r_arrived(c).wait_recv()
        out_t = out_t + rr_ref[c].astype(F32)
    out_ref[...] = (out_t.T * live_a * live_b).astype(BF16)

    for k in range(ny):
        m_first(k).wait_send()
    for k in range(1, ny):
        m_relay(k).wait_send()
    for k in range(nx):
        t_first(k).wait_send()
    for k in range(1, nx):
        t_relay(k).wait_send()
    for k in range(1, nb):
        for e in range(2):
            c_copy(k, mb, e).wait_send()
    for c in range(nc):
        f_copy(c).wait_send()
        x_copy(c).wait_send()
    for k in range(1, nc):
        r_copy(peer_chip(k)).wait_send()


def per_device(na, nb, amplitudes, code, counts, pair_irrep, integrals, one_body):
    ra, rb = amplitudes.shape
    pairs, ns = code.shape
    his = ns // 128
    tr = ns // (na * nb)
    dma = pltpu.SemaphoreType.DMA
    vmem = pl.BlockSpec(memory_space=pltpu.VMEM)
    return pl.pallas_call(
        functools.partial(kernel, na, nb, ns // counts.shape[0]),
        out_shape=jax.ShapeDtypeStruct((ra, rb), BF16),
        in_specs=[vmem] * 6,
        out_specs=vmem,
        scratch_shapes=[
            pltpu.VMEM((pairs, ns), F32),
            pltpu.VMEM((pairs, ns), F32),
            pltpu.VMEM((pairs, ns), F32),
            pltpu.VMEM((2, pairs, rb), F32),
            pltpu.VMEM((2, 2 * ra, ns // 4), BF16),
            pltpu.VMEM((2, rb, ra), BF16),
            pltpu.VMEM((pairs, ra, rb), F32),
            pltpu.VMEM((pairs, ra, rb), F32),
            pltpu.VMEM((pairs, rb, ra), BF16),
            pltpu.VMEM((pairs * 8, pairs * 8), BF16),
            pltpu.VMEM((8, ns), F32),
            pltpu.VMEM((nb, ra, rb), BF16),
            pltpu.VMEM((na, his, tr, 128), BF16),
            pltpu.VMEM((nb, 2, na // 4, 2, tr, 128), BF16),
            pltpu.VMEM((na // 2, rb, ra), F32),
            pltpu.VMEM((na // 2, rb, ra), F32),
            pltpu.VMEM((na // 2, rb, ra), F32),
            pltpu.VMEM((na // 2, rb, ra), BF16),
            pltpu.VMEM((na // 2, rb, ra), BF16),
            dma((nb,)), dma((nb,)), dma((na // 2,)), dma((na // 2,)), dma((na // 2,)), dma((na // 2,)), dma, dma,
            dma((nb, 2)), dma((nb, 2)), dma((na // 2,)), dma((na // 2,)), dma((na // 2,)), dma((na // 2,)),
        ],
        compiler_params=pltpu.CompilerParams(
            collective_id=0, has_side_effects=True, vmem_limit_bytes=56 * 1024 * 1024),
    )(amplitudes, code, counts.reshape(1, -1), pair_irrep.reshape(1, -1), integrals, one_body.reshape(1, -1))


def solution(mesh):
    placed = (P("aa", "ba"), P(), P(), P(), P(), P())
    body = functools.partial(per_device, mesh.shape["aa"], mesh.shape["ba"])
    return jax.shard_map(body, mesh=mesh, in_specs=placed, out_specs=P("aa", "ba"), check_vma=False)
```

```python
import functools

import jax
import jax.numpy as jnp
from jax import lax
from jax.experimental import pallas as pl
from jax.experimental.pallas import tpu as pltpu
from jax.sharding import PartitionSpec as P

F32 = jnp.float32
BF16 = jnp.bfloat16
MESH = pl.DeviceIdType.MESH
GATHER = 8
MIX = 8
LAG = 3


def iota(shape, axis):
    return lax.broadcasted_iota(jnp.int32, shape, axis)


def dot(a, b):
    return jnp.dot(a, b, preferred_element_type=F32)


def dot_nt(a, b):
    return lax.dot_general(a, b, (((1,), (1,)), ((), ())), preferred_element_type=F32)


def kernel(
    na, nb, capacity,
    amp_in, code_in, counts_in, irrep_in, integrals_in, one_body_in,
    out_ref,
    amp_ref, code_ref, counts_ref, irrep_ref, integrals_ref, one_body_ref, in_sem,
    hi_ref, lo_ref, sg_ref, kk_ref, m2_ref, mt_ref, y_ref, z_ref, zt_ref, kron_ref, live_ref,
    mg_ref, tb_ref, ta_ref, own_ref, xs_ref, xr_ref, rs_ref, rr_ref,
    m_send, m_recv, t_send, t_recv, f_send, f_recv, g_send, g_recv, c_send, c_recv, x_send, x_recv, r_send, r_recv,
):
    ra, rb = amp_ref.shape
    pairs, ns = code_ref.shape
    his = ns // 128
    half = his // 2
    tr = ns // (na * nb)
    keys = his * tr
    ma = lax.axis_index("aa")
    mb = lax.axis_index("ba")

    nc = na // 2
    chip = ma // 2
    core = lax.rem(ma, 2)
    sibling = chip * 2 + 1 - core

    nx = nc // 2
    ny = nb // 2
    z_hi = lax.rem(chip, 2)
    z_lo = lax.rem(mb, 2)

    def peer_chip(k):
        return lax.rem(chip + k, nc)

    def along_x(k, opposite):
        return lax.rem(chip // 2 + k, nx) * 2 + (1 - z_hi if opposite else z_hi)

    def along_y(k, opposite):
        return lax.rem(mb // 2 + k, ny) * 2 + (1 - z_lo if opposite else z_lo)

    def same_core(c):
        return c * 2 + core

    def peer_b(k):
        return lax.rem(mb + k, nb)

    barrier = pltpu.get_barrier_semaphore()
    for k in range(1, nb):
        pl.semaphore_signal(barrier, inc=1, device_id=(ma, peer_b(k)), device_id_type=MESH)
        pl.semaphore_signal(barrier, inc=1, device_id=(sibling, peer_b(k)), device_id_type=MESH)
    for k in range(1, nc):
        pl.semaphore_signal(barrier, inc=1, device_id=(same_core(peer_chip(k)), mb), device_id_type=MESH)
    pl.semaphore_signal(barrier, inc=1, device_id=(sibling, mb), device_id_type=MESH)
    loads = [
        pltpu.make_async_copy(src, dst, in_sem.at[i])
        for i, (src, dst) in enumerate((
            (amp_in, amp_ref), (code_in, code_ref), (counts_in, counts_ref), (irrep_in, irrep_ref),
            (integrals_in, integrals_ref), (one_body_in, one_body_ref)))
    ]
    for load in loads:
        load.start()
    loads[0].wait()
    pl.semaphore_wait(barrier, nc + 2 * (nb - 1))

    def m_copy(k, block, dest):
        return pltpu.make_async_remote_copy(
            src_ref=mg_ref.at[block], dst_ref=mg_ref.at[block], send_sem=m_send.at[k], recv_sem=m_recv.at[block],
            device_id=(ma, dest), device_id_type=MESH)

    def m_first(k):
        return pltpu.make_async_remote_copy(
            src_ref=amp_ref, dst_ref=mg_ref.at[mb], send_sem=m_send.at[k], recv_sem=m_recv.at[mb],
            device_id=(ma, along_y(k, k == 0)), device_id_type=MESH)

    def m_relay(k):
        return m_copy(ny + k, along_y(0, True), along_y(k, False))

    near = [k for k in range(1, ny) if k in (1, ny - 1)]
    far = [k for k in range(1, ny) if k not in near]
    for k in [0] + near + far:
        m_first(k).start()

    for load in loads[1:]:
        load.wait()

    code = code_ref[...]
    target = jnp.abs(code) - 1
    hi = lax.shift_right_arithmetic(target, 7)
    lo = target & 127
    sg = jnp.where(code > 0, 1.0, jnp.where(code < 0, -1.0, 0.0)).astype(F32)
    hi_ref[...] = hi.astype(F32)
    lo_ref[...] = lo.astype(F32)
    sg_ref[...] = sg

    blocks = counts_ref.shape[1]
    counts = jnp.broadcast_to(counts_ref[...].astype(F32), (8, blocks)).astype(BF16)
    spread = (iota((blocks, ns), 1) // capacity == iota((blocks, ns), 0)).astype(F32).astype(BF16)
    slots = (iota((8, ns), 1) % capacity).astype(F32)
    live8 = jnp.where(slots < dot(counts, spread), 1.0, 0.0)
    live = live8[0:1]
    live_ref[...] = live8

    irr = jnp.broadcast_to(irrep_ref[...], (pairs, pairs))
    eye = iota((pairs, pairs), 0) == iota((pairs, pairs), 1)
    irr_col = jnp.sum(jnp.where(eye, irr, 0), axis=1, keepdims=True)
    w = jnp.where(irr_col == irr, integrals_ref[...].astype(F32), 0.0).astype(BF16)
    w_t = dot_nt(eye.astype(F32).astype(BF16), w).astype(BF16)

    first = mb * rb + ma * tr
    base = pl.multiple_of((first // 128) * 128, 128)
    off = first - base
    n = pairs * tr
    own = jnp.concatenate(
        [hi_ref[:, pl.ds(base, 128)], lo_ref[:, pl.ds(base, 128)], sg_ref[:, pl.ds(base, 128)]], axis=0
    ).astype(BF16)
    pick = (iota((128, n), 0) == off + iota((128, n), 1) % tr).astype(F32).astype(BF16)
    mine = dot(own, pick)
    here = iota((pairs, n), 0) == iota((pairs, n), 1) // tr
    k_hi = jnp.sum(jnp.where(here, mine[0:pairs], 0.0), axis=0, keepdims=True)
    k_lo = jnp.sum(jnp.where(here, mine[pairs : 2 * pairs], 0.0), axis=0, keepdims=True)
    k_sg = jnp.sum(jnp.where(here, mine[2 * pairs :], 0.0), axis=0, keepdims=True)
    here_b = here.astype(F32).astype(BF16)
    w_wide = dot(w_t, here_b)
    o_wide = dot(jnp.broadcast_to(one_body_ref[...], (8, pairs)), here_b)[0:1]
    k_lo_b = k_lo.astype(BF16)
    iota128 = iota((128, n), 0).astype(F32).astype(BF16)
    one = jnp.ones((), BF16)
    zero = jnp.zeros((), BF16)
    planes = jnp.concatenate([hi_ref[...], lo_ref[...], sg_ref[...] * live], axis=0).astype(BF16)
    got = jnp.zeros((3 * pairs, n), F32)
    for h in range(0, his, 2):
        sel = []
        for e in range(2):
            loc = jnp.where(k_hi == float(h + e), k_lo, -1.0).astype(BF16)
            sel.append(jnp.where(iota128 == loc, one, zero))
        got = got + dot(planes[:, h * 128 : (h + 2) * 128], jnp.concatenate(sel, axis=0))
    row = (iota((pairs, n), 1) % tr).astype(F32)

    def split(high, low):
        upper = jnp.floor(high * 0.5)
        return upper * float(tr), (high - 2.0 * upper) * 128.0 + low

    key_all, low_all = split(got[0:pairs], got[pairs : 2 * pairs])
    key_all = (key_all + row).astype(BF16)
    val_all = (0.5 * w_wide * got[2 * pairs :] * k_sg).astype(BF16)
    key_one, low_one = split(k_hi, k_lo)
    key_one = (key_one + row[0:1]).astype(BF16)
    low_t = jnp.concatenate([low_all, jnp.broadcast_to(low_one, (8, n))], axis=0).T
    low_t = low_t.astype(BF16)
    iota_keys = iota((keys // 2, n), 0).astype(F32).astype(BF16)
    iota_low = iota((n, 256), 1).astype(F32).astype(BF16)

    def histogram(key, val, at):
        a = jnp.where(iota_keys == key, val, zero)
        hit = iota_low == jnp.broadcast_to(low_t[:, at : at + 1], (n, 256))
        b = jnp.where(hit, one, zero)
        return dot(a, b)

    t_acc = histogram(key_one, (o_wide * k_sg).astype(BF16), pairs)
    for q in range(pairs):
        t_acc = t_acc + histogram(key_all[q : q + 1], val_all[q : q + 1], q)
    t_acc = t_acc.astype(BF16)
    for h in range(2):
        part = t_acc[:, h * 128 : (h + 1) * 128].reshape(his // 2, tr, 128)
        for g in range(his // 2):
            tb_ref[ma, 2 * g + h] = part[g]

    def t_copy(k, c, dest):
        slot = same_core(c)
        return pltpu.make_async_remote_copy(
            src_ref=tb_ref.at[slot], dst_ref=tb_ref.at[slot], send_sem=t_send.at[k], recv_sem=t_recv.at[c],
            device_id=(same_core(dest), mb), device_id_type=MESH)

    def t_first(k):
        return t_copy(k, chip, along_x(k, k == 0))

    def t_relay(k):
        return t_copy(nx + k, along_x(0, True), along_x(k, False))

    def f_copy(c):
        slot = same_core(c)
        return pltpu.make_async_remote_copy(
            src_ref=tb_ref.at[slot], dst_ref=tb_ref.at[slot], send_sem=f_send.at[c], recv_sem=f_recv.at[c],
            device_id=(sibling, mb), device_id_type=MESH)

    def f_arrived(c):
        slot = c * 2 + 1 - core
        return pltpu.make_async_remote_copy(
            src_ref=tb_ref.at[slot], dst_ref=tb_ref.at[slot], send_sem=f_send.at[c], recv_sem=f_recv.at[c],
            device_id=(sibling, mb), device_id_type=MESH)

    hc = nc // 2
    lag = min(LAG, hc)

    def pass_on(c):
        for k in range(1, nb):
            pltpu.make_async_remote_copy(
                src_ref=tb_ref.at[same_core(c), pl.ds(chip * 2, 2)], dst_ref=ta_ref.at[mb, core, lax.rem(c, hc)],
                send_sem=c_send.at[k, c // hc], recv_sem=c_recv.at[mb, core],
                device_id=(chip * 2 + c // hc, peer_b(k)), device_id_type=MESH).start()

    def c_copy(k, src, e):
        return pltpu.make_async_remote_copy(
            src_ref=ta_ref.at[src, e], dst_ref=ta_ref.at[src, e], send_sem=c_send.at[k, e],
            recv_sem=c_recv.at[src, e], device_id=(chip * 2 + e, peer_b(k)), device_id_type=MESH)

    def hand_over(c):
        t_copy(0, c, chip).wait_recv()
        f_copy(c).start()
        pass_on(c)

    near_x = [k for k in range(1, nx) if k in (1, nx - 1)]
    far_x = [k for k in range(1, nx) if k not in near_x]
    for k in [0] + near_x + far_x:
        t_first(k).start()
    f_copy(chip).start()
    pass_on(chip)

    m_copy(0, along_y(0, True), mb).wait_recv()
    for k in near + far:
        m_relay(k).start()

    grow = (iota((pairs * 8, pairs), 0) // 8 == iota((pairs * 8, pairs), 1)).astype(F32).astype(BF16)
    wide = dot_nt(dot(grow, w).astype(BF16), grow)
    same = iota((pairs * 8, pairs * 8), 0) % 8 == iota((pairs * 8, pairs * 8), 1) % 8
    kron_ref[...] = jnp.where(same, wide, 0.0).astype(BF16)

    low_a = ma * ra
    block_of = (iota((ra, blocks), 0) + low_a) // capacity
    count_a = jnp.sum(
        jnp.where(block_of == iota((ra, blocks), 1), counts_ref[...].astype(F32), 0.0), axis=1, keepdims=True)
    live_a = jnp.where(((iota((ra, 1), 0) + low_a) % capacity).astype(F32) < count_a, 1.0, 0.0)
    mg_ref[mb] = amp_ref[...]
    low_b = pl.multiple_of(mb * rb, 128)
    live_b = live_ref[0:1, pl.ds(low_b, rb)]
    mine_f = amp_ref[...].astype(F32) * live_a * live_b
    mt_ref[core] = mine_f.T.astype(BF16)
    g_copy = pltpu.make_async_remote_copy(
        src_ref=mt_ref.at[core], dst_ref=mt_ref.at[core], send_sem=g_send, recv_sem=g_recv,
        device_id=(sibling, mb), device_id_type=MESH)
    g_copy.start()

    hi_b = hi_ref[:, pl.ds(low_b, rb)]
    y_b = jnp.floor(hi_b * 0.25)
    rest_b = hi_b - 4.0 * y_b
    for turn in range(2):
        e_b = rest_b - 2.0 * (1 - z_lo if turn else z_lo).astype(F32)
        inside = (e_b >= 0.0) & (e_b < 2.0)
        kk_ref[turn] = jnp.where(inside, 2.0 * y_b + e_b, -1.0)

    iota_b = iota((128, rb), 0).astype(F32).astype(BF16)

    def arrange(turn):
        for y in range(ny):
            block = 2 * y + (1 - z_lo if turn else z_lo)
            on = live_ref[0:1, pl.ds(pl.multiple_of(block * rb, 128), rb)]
            part = (mg_ref[block].astype(F32) * live_a * on).astype(BF16)
            for e in range(2):
                u = 2 * y + e
                h, at = u // ny, (u % ny) * 128
                m2_ref[turn, h * ra : (h + 1) * ra, at : at + 128] = part[:, e * 128 : (e + 1) * 128]

    def gather_one(turn, q):
        kk_q = kk_ref[turn, pl.ds(q, 1), :]
        lo_q = lo_ref[pl.ds(q, 1), pl.ds(low_b, rb)]
        sg_q = sg_ref[pl.ds(q, 1), pl.ds(low_b, rb)]
        upper = kk_q >= float(ny)
        inner = jnp.where(upper, kk_q - float(ny), kk_q)
        hots = []
        for j in range(ny):
            loc = jnp.where(inner == float(j), lo_q, -1.0).astype(BF16)
            hots.append(jnp.where(iota_b == loc, one, zero))
        got_q = dot(m2_ref[turn], jnp.concatenate(hots, axis=0))
        picked = jnp.where(jnp.broadcast_to(upper, (ra, rb)), got_q[ra:], got_q[:ra]) * (sg_q * live_b)
        if turn:
            z_ref[q] = (y_ref[q] + picked).astype(BF16).T.astype(F32)
        else:
            y_ref[q] = picked

    trips = pairs // GATHER

    for k in range(1, ny):
        m_copy(0, along_y(k, False), mb).wait_recv()
    arrange(0)

    def gather_own(i, carry):
        for e in range(GATHER):
            gather_one(0, i * GATHER + e)

        @pl.when(i == trips - 2)
        def _():
            t_copy(0, along_x(0, True), chip).wait_recv()
            for k in near_x + far_x:
                t_relay(k).start()
            f_copy(along_x(0, True)).start()
            pass_on(along_x(0, True))
        return carry

    lax.fori_loop(0, trips, gather_own, 0)
    for k in near_x + far_x:
        hand_over(along_x(k, False))
    for k in range(1, ny):
        m_copy(0, along_y(k, True), mb).wait_recv()
    arrange(1)

    def gather_other(i, carry):
        for e in range(GATHER):
            gather_one(1, i * GATHER + e)

        return carry

    lax.fori_loop(0, trips, gather_other, 0)
    for k in near_x:
        hand_over(along_x(k, True))

    def mix(i, carry):
        for e in range(MIX):
            at = pl.multiple_of((i * MIX + e) * 16, 16)
            rows = [z_ref[:, pl.ds(at + 8 * h, 8), :].reshape(pairs * 8, ra) for h in range(2)]
            mixed = dot(kron_ref[...], jnp.concatenate(rows, axis=1).astype(BF16)).reshape(pairs, 8, 2 * ra)
            zt_ref[:, pl.ds(at, 16), :] = jnp.concatenate([mixed[:, :, :ra], mixed[:, :, ra:]], axis=1).astype(BF16)
        return carry

    lax.fori_loop(0, rb // 16 // MIX, mix, 0)
    for k in far_x:
        hand_over(along_x(k, True))


    width = 2 * ra
    group = min(pairs, 8)

    def x_copy(c):
        return pltpu.make_async_remote_copy(
            src_ref=xs_ref.at[c], dst_ref=xr_ref.at[c], send_sem=x_send.at[c], recv_sem=x_recv.at[c],
            device_id=(sibling, mb), device_id_type=MESH)

    def r_copy(c):
        return pltpu.make_async_remote_copy(
            src_ref=rs_ref.at[c], dst_ref=rr_ref.at[chip], send_sem=r_send.at[c], recv_sem=r_recv.at[chip],
            device_id=(same_core(c), mb), device_id_type=MESH)

    def r_arrived(c):
        return pltpu.make_async_remote_copy(
            src_ref=rs_ref.at[c], dst_ref=rr_ref.at[c], send_sem=r_send.at[c], recv_sem=r_recv.at[c],
            device_id=(same_core(c), mb), device_id_type=MESH)

    def scatter(i, carry):
        d = turn_of(i)
        at = pl.multiple_of(d * width, 128)
        acc = jnp.zeros((rb, width), F32)
        for p0 in range(0, pairs, group):
            hots = []
            for p in range(p0, p0 + group):
                hit = hi_ref[p : p + 1, pl.ds(at, width)] == ma.astype(F32)
                loc = jnp.where(hit, lo_ref[p : p + 1, pl.ds(at, width)], -1.0).astype(BF16)
                hots.append(jnp.where(iota_b == loc, sg_ref[p : p + 1, pl.ds(at, width)].astype(BF16), zero))
            lhs = jnp.concatenate([zt_ref[p] for p in range(p0, p0 + group)], axis=1)
            acc = acc + dot(lhs, jnp.concatenate(hots, axis=0))
        first_core = core == 0
        own_ref[d] = jnp.where(first_core, acc[:, :ra], acc[:, ra:])
        xs_ref[d] = jnp.where(first_core, acc[:, ra:], acc[:, :ra])
        x_copy(d).start()

        @pl.when(i == lag - 1)
        def _():
            for c in range(nc):
                f_arrived(c).wait_recv()
            for e in range(2):
                for c in range(hc):
                    ta_ref[mb, e, c] = tb_ref[core * nc + 2 * c + e, pl.ds(chip * 2, 2)]
            g_copy.wait()

        @pl.when(i >= lag)
        def _():
            send(turn_of(i - lag))

        @pl.when(i == nc - 1)
        def _():
            if lag > 1:
                send(turn_of(nc - lag))
        return carry

    def turn_of(i):
        return lax.rem(chip // 2 + nx - 1 - lax.rem(i, nx), nx) * 2 + jnp.where(i < nx, 1 - z_hi, z_hi)

    def arrival(i):
        return lax.rem(chip // 2 + 1 + i % nx, nx) * 2 + (1 - z_hi if i < nx else z_hi)

    def summed(d):
        @pl.when(d != mb)
        def _():
            for e in range(2):
                c_copy(1, d, e).wait_recv()
        x_copy(d).wait_recv()
        acc = own_ref[d] + xr_ref[d]
        for h in range(2):
            rows = jnp.concatenate([ta_ref[d, e, c, h] for c in range(hc) for e in range(2)], axis=0)
            acc = acc + dot_nt(mt_ref[h], rows)
        return acc

    def send(d):
        rs_ref[d] = summed(d).astype(BF16)
        r_copy(d).start()

    lax.fori_loop(0, nc, scatter, 0)
    for i in range(nc - lag + 1, nc - 1):
        send(turn_of(i))

    res = jnp.zeros((rb, ra), F32)
    for turn in range(2):
        for u in range(0, 2 * ny, min(ny, 2)):
            parts = []
            for v in range(u, u + min(ny, 2)):
                h = 4 * (v // 2) + 2 * (1 - z_lo if turn else z_lo) + v % 2
                parts.append(tb_ref[:, h].reshape(rb, 128))
            h, at = u // ny, (u % ny) * 128
            res = res + dot_nt(
                jnp.concatenate(parts, axis=1), m2_ref[turn, h * ra : (h + 1) * ra, at : at + 128 * len(parts)])


    out_t = res + summed(chip)
    for i in range(nc - 1):
        c = arrival(i)
        r_arrived(c).wait_recv()
        out_t = out_t + rr_ref[c].astype(F32)
    out_ref[...] = (out_t.T * live_a * live_b).astype(BF16)

    for k in range(ny):
        m_first(k).wait_send()
    for k in range(1, ny):
        m_relay(k).wait_send()
    for k in range(nx):
        t_first(k).wait_send()
    for k in range(1, nx):
        t_relay(k).wait_send()
    for k in range(1, nb):
        for e in range(2):
            c_copy(k, mb, e).wait_send()
    for c in range(nc):
        f_copy(c).wait_send()
        x_copy(c).wait_send()
    for k in range(1, nc):
        r_copy(peer_chip(k)).wait_send()


def per_device(na, nb, amplitudes, code, counts, pair_irrep, integrals, one_body):
    ra, rb = amplitudes.shape
    pairs, ns = code.shape
    his = ns // 128
    tr = ns // (na * nb)
    dma = pltpu.SemaphoreType.DMA
    vmem = pl.BlockSpec(memory_space=pltpu.VMEM)
    return pl.pallas_call(
        functools.partial(kernel, na, nb, ns // counts.shape[0]),
        out_shape=jax.ShapeDtypeStruct((ra, rb), BF16),
        in_specs=[pl.BlockSpec(memory_space=pl.ANY)] * 6,
        out_specs=vmem,
        scratch_shapes=[
            pltpu.VMEM((ra, rb), BF16),
            pltpu.VMEM((pairs, ns), jnp.int32),
            pltpu.VMEM((1, counts.shape[0]), jnp.int32),
            pltpu.VMEM((1, pairs), jnp.int32),
            pltpu.VMEM((pairs, pairs), BF16),
            pltpu.VMEM((1, pairs), BF16),
            dma((6,)),
            pltpu.VMEM((pairs, ns), F32),
            pltpu.VMEM((pairs, ns), F32),
            pltpu.VMEM((pairs, ns), F32),
            pltpu.VMEM((2, pairs, rb), F32),
            pltpu.VMEM((2, 2 * ra, ns // 4), BF16),
            pltpu.VMEM((2, rb, ra), BF16),
            pltpu.VMEM((pairs, ra, rb), F32),
            pltpu.VMEM((pairs, rb, ra), F32),
            pltpu.VMEM((pairs, rb, ra), BF16),
            pltpu.VMEM((pairs * 8, pairs * 8), BF16),
            pltpu.VMEM((8, ns), F32),
            pltpu.VMEM((nb, ra, rb), BF16),
            pltpu.VMEM((na, his, tr, 128), BF16),
            pltpu.VMEM((nb, 2, na // 4, 2, tr, 128), BF16),
            pltpu.VMEM((na // 2, rb, ra), F32),
            pltpu.VMEM((na // 2, rb, ra), F32),
            pltpu.VMEM((na // 2, rb, ra), F32),
            pltpu.VMEM((na // 2, rb, ra), BF16),
            pltpu.VMEM((na // 2, rb, ra), BF16),
            dma((nb,)), dma((nb,)), dma((na // 2,)), dma((na // 2,)), dma((na // 2,)), dma((na // 2,)), dma, dma,
            dma((nb, 2)), dma((nb, 2)), dma((na // 2,)), dma((na // 2,)), dma((na // 2,)), dma((na // 2,)),
        ],
        compiler_params=pltpu.CompilerParams(
            collective_id=0, has_side_effects=True, vmem_limit_bytes=56 * 1024 * 1024),
    )(amplitudes, code, counts.reshape(1, -1), pair_irrep.reshape(1, -1), integrals, one_body.reshape(1, -1))


def solution(mesh):
    placed = (P("aa", "ba"), P(), P(), P(), P(), P())
    body = functools.partial(per_device, mesh.shape["aa"], mesh.shape["ba"])
    return jax.shard_map(body, mesh=mesh, in_specs=placed, out_specs=P("aa", "ba"), check_vma=False)
```

```python
import functools

import jax
import jax.numpy as jnp
from jax import lax
from jax.experimental import pallas as pl
from jax.experimental.pallas import tpu as pltpu
from jax.sharding import PartitionSpec as P

F32 = jnp.float32
BF16 = jnp.bfloat16
MESH = pl.DeviceIdType.MESH
GATHER = 8
MIX = 16
LAG = 3


def iota(shape, axis):
    return lax.broadcasted_iota(jnp.int32, shape, axis)


def dot(a, b):
    return jnp.dot(a, b, preferred_element_type=F32)


def dot_nt(a, b):
    return lax.dot_general(a, b, (((1,), (1,)), ((), ())), preferred_element_type=F32)


def kernel(
    na, nb, capacity,
    amp_in, code_in, counts_in, irrep_in, integrals_in, one_body_in,
    out_ref,
    amp_ref, code_ref, counts_ref, irrep_ref, integrals_ref, one_body_ref, in_sem,
    hi_ref, lo_ref, sg_ref, kk_ref, m2_ref, mt_ref, y_ref, z_ref, zt_ref, kron_ref, live_ref,
    mg_ref, tb_ref, ta_ref, own_ref, xs_ref, xr_ref, rs_ref, rr_ref,
    m_send, m_recv, t_send, t_recv, f_send, f_recv, g_send, g_recv, c_send, c_recv, x_send, x_recv, r_send, r_recv,
):
    ra, rb = amp_ref.shape
    pairs, ns = code_ref.shape
    his = ns // 128
    half = his // 2
    tr = ns // (na * nb)
    keys = his * tr
    ma = lax.axis_index("aa")
    mb = lax.axis_index("ba")

    nc = na // 2
    chip = ma // 2
    core = lax.rem(ma, 2)
    sibling = chip * 2 + 1 - core

    nx = nc // 2
    ny = nb // 2
    z_hi = lax.rem(chip, 2)
    z_lo = lax.rem(mb, 2)

    def peer_chip(k):
        return lax.rem(chip + k, nc)

    def along_x(k, opposite):
        return lax.rem(chip // 2 + k, nx) * 2 + (1 - z_hi if opposite else z_hi)

    def along_y(k, opposite):
        return lax.rem(mb // 2 + k, ny) * 2 + (1 - z_lo if opposite else z_lo)

    def same_core(c):
        return c * 2 + core

    def peer_b(k):
        return lax.rem(mb + k, nb)

    barrier = pltpu.get_barrier_semaphore()
    for k in range(1, nb):
        pl.semaphore_signal(barrier, inc=1, device_id=(ma, peer_b(k)), device_id_type=MESH)
        pl.semaphore_signal(barrier, inc=1, device_id=(sibling, peer_b(k)), device_id_type=MESH)
    for k in range(1, nc):
        pl.semaphore_signal(barrier, inc=1, device_id=(same_core(peer_chip(k)), mb), device_id_type=MESH)
    pl.semaphore_signal(barrier, inc=1, device_id=(sibling, mb), device_id_type=MESH)
    loads = [
        pltpu.make_async_copy(src, dst, in_sem.at[i])
        for i, (src, dst) in enumerate((
            (amp_in, amp_ref), (code_in, code_ref), (counts_in, counts_ref), (irrep_in, irrep_ref),
            (integrals_in, integrals_ref), (one_body_in, one_body_ref)))
    ]
    for load in loads:
        load.start()
    loads[0].wait()
    pl.semaphore_wait(barrier, nc + 2 * (nb - 1))

    def m_copy(k, block, dest):
        return pltpu.make_async_remote_copy(
            src_ref=mg_ref.at[block], dst_ref=mg_ref.at[block], send_sem=m_send.at[k], recv_sem=m_recv.at[block],
            device_id=(ma, dest), device_id_type=MESH)

    def m_first(k):
        return pltpu.make_async_remote_copy(
            src_ref=amp_ref, dst_ref=mg_ref.at[mb], send_sem=m_send.at[k], recv_sem=m_recv.at[mb],
            device_id=(ma, along_y(k, k == 0)), device_id_type=MESH)

    def m_relay(k):
        return m_copy(ny + k, along_y(0, True), along_y(k, False))

    near = [k for k in range(1, ny) if k in (1, ny - 1)]
    far = [k for k in range(1, ny) if k not in near]
    for k in [0] + near + far:
        m_first(k).start()

    for load in loads[1:]:
        load.wait()

    code = code_ref[...]
    target = jnp.abs(code) - 1
    hi = lax.shift_right_arithmetic(target, 7)
    lo = target & 127
    sg = jnp.where(code > 0, 1.0, jnp.where(code < 0, -1.0, 0.0)).astype(F32)
    hi_ref[...] = hi.astype(F32)
    lo_ref[...] = lo.astype(F32)
    sg_ref[...] = sg

    blocks = counts_ref.shape[1]
    counts = jnp.broadcast_to(counts_ref[...].astype(F32), (8, blocks)).astype(BF16)
    spread = (iota((blocks, ns), 1) // capacity == iota((blocks, ns), 0)).astype(F32).astype(BF16)
    slots = (iota((8, ns), 1) % capacity).astype(F32)
    live8 = jnp.where(slots < dot(counts, spread), 1.0, 0.0)
    live = live8[0:1]
    live_ref[...] = live8

    irr = jnp.broadcast_to(irrep_ref[...], (pairs, pairs))
    eye = iota((pairs, pairs), 0) == iota((pairs, pairs), 1)
    irr_col = jnp.sum(jnp.where(eye, irr, 0), axis=1, keepdims=True)
    w = jnp.where(irr_col == irr, integrals_ref[...].astype(F32), 0.0).astype(BF16)
    w_t = dot_nt(eye.astype(F32).astype(BF16), w).astype(BF16)

    first = mb * rb + ma * tr
    base = pl.multiple_of((first // 128) * 128, 128)
    off = first - base
    n = pairs * tr
    own = jnp.concatenate(
        [hi_ref[:, pl.ds(base, 128)], lo_ref[:, pl.ds(base, 128)], sg_ref[:, pl.ds(base, 128)]], axis=0
    ).astype(BF16)
    pick = (iota((128, n), 0) == off + iota((128, n), 1) % tr).astype(F32).astype(BF16)
    mine = dot(own, pick)
    here = iota((pairs, n), 0) == iota((pairs, n), 1) // tr
    k_hi = jnp.sum(jnp.where(here, mine[0:pairs], 0.0), axis=0, keepdims=True)
    k_lo = jnp.sum(jnp.where(here, mine[pairs : 2 * pairs], 0.0), axis=0, keepdims=True)
    k_sg = jnp.sum(jnp.where(here, mine[2 * pairs :], 0.0), axis=0, keepdims=True)
    here_b = here.astype(F32).astype(BF16)
    w_wide = dot(w_t, here_b)
    o_wide = dot(jnp.broadcast_to(one_body_ref[...], (8, pairs)), here_b)[0:1]
    k_lo_b = k_lo.astype(BF16)
    iota128 = iota((128, n), 0).astype(F32).astype(BF16)
    one = jnp.ones((), BF16)
    zero = jnp.zeros((), BF16)
    planes = jnp.concatenate([hi_ref[...], lo_ref[...], sg_ref[...] * live], axis=0).astype(BF16)
    got = jnp.zeros((3 * pairs, n), F32)
    for h in range(0, his, 2):
        sel = []
        for e in range(2):
            loc = jnp.where(k_hi == float(h + e), k_lo, -1.0).astype(BF16)
            sel.append(jnp.where(iota128 == loc, one, zero))
        got = got + dot(planes[:, h * 128 : (h + 2) * 128], jnp.concatenate(sel, axis=0))
    row = (iota((pairs, n), 1) % tr).astype(F32)

    def split(high, low):
        upper = jnp.floor(high * 0.5)
        return upper * float(tr), (high - 2.0 * upper) * 128.0 + low

    key_all, low_all = split(got[0:pairs], got[pairs : 2 * pairs])
    key_all = (key_all + row).astype(BF16)
    val_all = (0.5 * w_wide * got[2 * pairs :] * k_sg).astype(BF16)
    key_one, low_one = split(k_hi, k_lo)
    key_one = (key_one + row[0:1]).astype(BF16)
    low_t = jnp.concatenate([low_all, jnp.broadcast_to(low_one, (8, n))], axis=0).T
    low_t = low_t.astype(BF16)
    iota_keys = iota((keys // 2, n), 0).astype(F32).astype(BF16)
    iota_low = iota((n, 256), 1).astype(F32).astype(BF16)

    def histogram(key, val, at):
        a = jnp.where(iota_keys == key, val, zero)
        hit = iota_low == jnp.broadcast_to(low_t[:, at : at + 1], (n, 256))
        b = jnp.where(hit, one, zero)
        return dot(a, b)

    t_acc = histogram(key_one, (o_wide * k_sg).astype(BF16), pairs)
    for q in range(pairs):
        t_acc = t_acc + histogram(key_all[q : q + 1], val_all[q : q + 1], q)
    t_acc = t_acc.astype(BF16)
    for h in range(2):
        part = t_acc[:, h * 128 : (h + 1) * 128].reshape(his // 2, tr, 128)
        for g in range(his // 2):
            tb_ref[ma, 2 * g + h] = part[g]

    def t_copy(k, c, dest):
        slot = same_core(c)
        return pltpu.make_async_remote_copy(
            src_ref=tb_ref.at[slot], dst_ref=tb_ref.at[slot], send_sem=t_send.at[k], recv_sem=t_recv.at[c],
            device_id=(same_core(dest), mb), device_id_type=MESH)

    def t_first(k):
        return t_copy(k, chip, along_x(k, k == 0))

    def t_relay(k):
        return t_copy(nx + k, along_x(0, True), along_x(k, False))

    def f_copy(c):
        slot = same_core(c)
        return pltpu.make_async_remote_copy(
            src_ref=tb_ref.at[slot], dst_ref=tb_ref.at[slot], send_sem=f_send.at[c], recv_sem=f_recv.at[c],
            device_id=(sibling, mb), device_id_type=MESH)

    def f_arrived(c):
        slot = c * 2 + 1 - core
        return pltpu.make_async_remote_copy(
            src_ref=tb_ref.at[slot], dst_ref=tb_ref.at[slot], send_sem=f_send.at[c], recv_sem=f_recv.at[c],
            device_id=(sibling, mb), device_id_type=MESH)

    hc = nc // 2
    lag = min(LAG, hc)

    def pass_on(c):
        for k in range(1, nb):
            pltpu.make_async_remote_copy(
                src_ref=tb_ref.at[same_core(c), pl.ds(chip * 2, 2)], dst_ref=ta_ref.at[mb, core, lax.rem(c, hc)],
                send_sem=c_send.at[k, c // hc], recv_sem=c_recv.at[mb, core],
                device_id=(chip * 2 + c // hc, peer_b(k)), device_id_type=MESH).start()

    def c_copy(k, src, e):
        return pltpu.make_async_remote_copy(
            src_ref=ta_ref.at[src, e], dst_ref=ta_ref.at[src, e], send_sem=c_send.at[k, e],
            recv_sem=c_recv.at[src, e], device_id=(chip * 2 + e, peer_b(k)), device_id_type=MESH)

    def hand_over(c):
        t_copy(0, c, chip).wait_recv()
        f_copy(c).start()
        pass_on(c)

    near_x = [k for k in range(1, nx) if k in (1, nx - 1)]
    far_x = [k for k in range(1, nx) if k not in near_x]
    for k in [0] + near_x + far_x:
        t_first(k).start()
    f_copy(chip).start()
    pass_on(chip)

    m_copy(0, along_y(0, True), mb).wait_recv()
    for k in near + far:
        m_relay(k).start()

    grow = (iota((pairs * 8, pairs), 0) // 8 == iota((pairs * 8, pairs), 1)).astype(F32).astype(BF16)
    wide = dot_nt(dot(grow, w).astype(BF16), grow)
    same = iota((pairs * 8, pairs * 8), 0) % 8 == iota((pairs * 8, pairs * 8), 1) % 8
    kron_ref[...] = jnp.where(same, wide, 0.0).astype(BF16)

    low_a = ma * ra
    block_of = (iota((ra, blocks), 0) + low_a) // capacity
    count_a = jnp.sum(
        jnp.where(block_of == iota((ra, blocks), 1), counts_ref[...].astype(F32), 0.0), axis=1, keepdims=True)
    live_a = jnp.where(((iota((ra, 1), 0) + low_a) % capacity).astype(F32) < count_a, 1.0, 0.0)
    mg_ref[mb] = amp_ref[...]
    low_b = pl.multiple_of(mb * rb, 128)
    live_b = live_ref[0:1, pl.ds(low_b, rb)]
    mine_f = amp_ref[...].astype(F32) * live_a * live_b
    mt_ref[core] = mine_f.T.astype(BF16)
    g_copy = pltpu.make_async_remote_copy(
        src_ref=mt_ref.at[core], dst_ref=mt_ref.at[core], send_sem=g_send, recv_sem=g_recv,
        device_id=(sibling, mb), device_id_type=MESH)
    g_copy.start()

    hi_b = hi_ref[:, pl.ds(low_b, rb)]
    y_b = jnp.floor(hi_b * 0.25)
    rest_b = hi_b - 4.0 * y_b
    for turn in range(2):
        e_b = rest_b - 2.0 * (1 - z_lo if turn else z_lo).astype(F32)
        inside = (e_b >= 0.0) & (e_b < 2.0)
        kk_ref[turn] = jnp.where(inside, 2.0 * y_b + e_b, -1.0)

    iota_b = iota((128, rb), 0).astype(F32).astype(BF16)

    def arrange(turn):
        for y in range(ny):
            block = 2 * y + (1 - z_lo if turn else z_lo)
            on = live_ref[0:1, pl.ds(pl.multiple_of(block * rb, 128), rb)]
            part = (mg_ref[block].astype(F32) * live_a * on).astype(BF16)
            for e in range(2):
                u = 2 * y + e
                h, at = u // ny, (u % ny) * 128
                m2_ref[turn, h * ra : (h + 1) * ra, at : at + 128] = part[:, e * 128 : (e + 1) * 128]

    def gather_one(turn, q):
        kk_q = kk_ref[turn, pl.ds(q, 1), :]
        lo_q = lo_ref[pl.ds(q, 1), pl.ds(low_b, rb)]
        sg_q = sg_ref[pl.ds(q, 1), pl.ds(low_b, rb)]
        upper = kk_q >= float(ny)
        inner = jnp.where(upper, kk_q - float(ny), kk_q)
        hots = []
        for j in range(ny):
            loc = jnp.where(inner == float(j), lo_q, -1.0).astype(BF16)
            hots.append(jnp.where(iota_b == loc, one, zero))
        got_q = dot(m2_ref[turn], jnp.concatenate(hots, axis=0))
        picked = jnp.where(jnp.broadcast_to(upper, (ra, rb)), got_q[ra:], got_q[:ra]) * (sg_q * live_b)
        if turn:
            z_ref[q] = (y_ref[q] + picked).astype(BF16).T.astype(F32)
        else:
            y_ref[q] = picked

    trips = pairs // GATHER

    for k in range(1, ny):
        m_copy(0, along_y(k, False), mb).wait_recv()
    arrange(0)

    def gather_own(i, carry):
        for e in range(GATHER):
            gather_one(0, i * GATHER + e)

        @pl.when(i == trips - 3)
        def _():
            t_copy(0, along_x(0, True), chip).wait_recv()
            for k in near_x + far_x:
                t_relay(k).start()
            f_copy(along_x(0, True)).start()
            pass_on(along_x(0, True))
        return carry

    lax.fori_loop(0, trips, gather_own, 0)
    for k in near_x + far_x:
        hand_over(along_x(k, False))
    for k in range(1, ny):
        m_copy(0, along_y(k, True), mb).wait_recv()
    arrange(1)

    def gather_other(i, carry):
        for e in range(GATHER):
            gather_one(1, i * GATHER + e)

        @pl.when(i == trips - 2)
        def _():
            for k in near_x:
                hand_over(along_x(k, True))
        return carry

    lax.fori_loop(0, trips, gather_other, 0)
    for k in far_x:
        hand_over(along_x(k, True))

    def mix(i, carry):
        for e in range(MIX):
            at = pl.multiple_of((i * MIX + e) * 16, 16)
            rows = [z_ref[:, pl.ds(at + 8 * h, 8), :].reshape(pairs * 8, ra) for h in range(2)]
            mixed = dot(kron_ref[...], jnp.concatenate(rows, axis=1).astype(BF16)).reshape(pairs, 8, 2 * ra)
            zt_ref[:, pl.ds(at, 16), :] = jnp.concatenate([mixed[:, :, :ra], mixed[:, :, ra:]], axis=1).astype(BF16)
        return carry

    lax.fori_loop(0, rb // 16 // MIX, mix, 0)


    width = 2 * ra
    group = min(pairs, 8)

    def x_copy(c):
        return pltpu.make_async_remote_copy(
            src_ref=xs_ref.at[c], dst_ref=xr_ref.at[c], send_sem=x_send.at[c], recv_sem=x_recv.at[c],
            device_id=(sibling, mb), device_id_type=MESH)

    def r_copy(c):
        return pltpu.make_async_remote_copy(
            src_ref=rs_ref.at[c], dst_ref=rr_ref.at[chip], send_sem=r_send.at[c], recv_sem=r_recv.at[chip],
            device_id=(same_core(c), mb), device_id_type=MESH)

    def r_arrived(c):
        return pltpu.make_async_remote_copy(
            src_ref=rs_ref.at[c], dst_ref=rr_ref.at[c], send_sem=r_send.at[c], recv_sem=r_recv.at[c],
            device_id=(same_core(c), mb), device_id_type=MESH)

    def scatter(i, carry):
        d = turn_of(i)
        at = pl.multiple_of(d * width, 128)
        acc = jnp.zeros((rb, width), F32)
        for p0 in range(0, pairs, group):
            hots = []
            for p in range(p0, p0 + group):
                hit = hi_ref[p : p + 1, pl.ds(at, width)] == ma.astype(F32)
                loc = jnp.where(hit, lo_ref[p : p + 1, pl.ds(at, width)], -1.0).astype(BF16)
                hots.append(jnp.where(iota_b == loc, sg_ref[p : p + 1, pl.ds(at, width)].astype(BF16), zero))
            lhs = jnp.concatenate([zt_ref[p] for p in range(p0, p0 + group)], axis=1)
            acc = acc + dot(lhs, jnp.concatenate(hots, axis=0))
        first_core = core == 0
        own_ref[d] = jnp.where(first_core, acc[:, :ra], acc[:, ra:])
        xs_ref[d] = jnp.where(first_core, acc[:, ra:], acc[:, :ra])
        x_copy(d).start()

        @pl.when(i == lag - 1)
        def _():
            for c in range(nc):
                f_arrived(c).wait_recv()
            for e in range(2):
                for c in range(hc):
                    ta_ref[mb, e, c] = tb_ref[core * nc + 2 * c + e, pl.ds(chip * 2, 2)]
            g_copy.wait()

        @pl.when(i >= lag)
        def _():
            send(turn_of(i - lag))

        @pl.when(i == nc - 1)
        def _():
            if lag > 1:
                send(turn_of(nc - lag))
        return carry

    def turn_of(i):
        return lax.rem(chip // 2 + nx - 1 - lax.rem(i, nx), nx) * 2 + jnp.where(i < nx, 1 - z_hi, z_hi)

    def arrival(i):
        return lax.rem(chip // 2 + 1 + i % nx, nx) * 2 + (1 - z_hi if i < nx else z_hi)

    def summed(d):
        @pl.when(d != mb)
        def _():
            for e in range(2):
                c_copy(1, d, e).wait_recv()
        x_copy(d).wait_recv()
        acc = own_ref[d] + xr_ref[d]
        for h in range(2):
            rows = jnp.concatenate([ta_ref[d, e, c, h] for c in range(hc) for e in range(2)], axis=0)
            acc = acc + dot_nt(mt_ref[h], rows)
        return acc

    def send(d):
        rs_ref[d] = summed(d).astype(BF16)
        r_copy(d).start()

    lax.fori_loop(0, nc, scatter, 0)
    for i in range(nc - lag + 1, nc - 1):
        send(turn_of(i))

    res = jnp.zeros((rb, ra), F32)
    for turn in range(2):
        for u in range(0, 2 * ny, min(ny, 2)):
            parts = []
            for v in range(u, u + min(ny, 2)):
                h = 4 * (v // 2) + 2 * (1 - z_lo if turn else z_lo) + v % 2
                parts.append(tb_ref[:, h].reshape(rb, 128))
            h, at = u // ny, (u % ny) * 128
            res = res + dot_nt(
                jnp.concatenate(parts, axis=1), m2_ref[turn, h * ra : (h + 1) * ra, at : at + 128 * len(parts)])


    out_t = res + summed(chip)
    for i in range(nc - 1):
        c = arrival(i)
        r_arrived(c).wait_recv()
        out_t = out_t + rr_ref[c].astype(F32)
    out_ref[...] = (out_t.T * live_a * live_b).astype(BF16)

    for k in range(ny):
        m_first(k).wait_send()
    for k in range(1, ny):
        m_relay(k).wait_send()
    for k in range(nx):
        t_first(k).wait_send()
    for k in range(1, nx):
        t_relay(k).wait_send()
    for k in range(1, nb):
        for e in range(2):
            c_copy(k, mb, e).wait_send()
    for c in range(nc):
        f_copy(c).wait_send()
        x_copy(c).wait_send()
    for k in range(1, nc):
        r_copy(peer_chip(k)).wait_send()


def per_device(na, nb, amplitudes, code, counts, pair_irrep, integrals, one_body):
    ra, rb = amplitudes.shape
    pairs, ns = code.shape
    his = ns // 128
    tr = ns // (na * nb)
    dma = pltpu.SemaphoreType.DMA
    vmem = pl.BlockSpec(memory_space=pltpu.VMEM)
    return pl.pallas_call(
        functools.partial(kernel, na, nb, ns // counts.shape[0]),
        out_shape=jax.ShapeDtypeStruct((ra, rb), BF16),
        in_specs=[pl.BlockSpec(memory_space=pl.ANY)] * 6,
        out_specs=vmem,
        scratch_shapes=[
            pltpu.VMEM((ra, rb), BF16),
            pltpu.VMEM((pairs, ns), jnp.int32),
            pltpu.VMEM((1, counts.shape[0]), jnp.int32),
            pltpu.VMEM((1, pairs), jnp.int32),
            pltpu.VMEM((pairs, pairs), BF16),
            pltpu.VMEM((1, pairs), BF16),
            dma((6,)),
            pltpu.VMEM((pairs, ns), F32),
            pltpu.VMEM((pairs, ns), F32),
            pltpu.VMEM((pairs, ns), F32),
            pltpu.VMEM((2, pairs, rb), F32),
            pltpu.VMEM((2, 2 * ra, ns // 4), BF16),
            pltpu.VMEM((2, rb, ra), BF16),
            pltpu.VMEM((pairs, ra, rb), F32),
            pltpu.VMEM((pairs, rb, ra), F32),
            pltpu.VMEM((pairs, rb, ra), BF16),
            pltpu.VMEM((pairs * 8, pairs * 8), BF16),
            pltpu.VMEM((8, ns), F32),
            pltpu.VMEM((nb, ra, rb), BF16),
            pltpu.VMEM((na, his, tr, 128), BF16),
            pltpu.VMEM((nb, 2, na // 4, 2, tr, 128), BF16),
            pltpu.VMEM((na // 2, rb, ra), F32),
            pltpu.VMEM((na // 2, rb, ra), F32),
            pltpu.VMEM((na // 2, rb, ra), F32),
            pltpu.VMEM((na // 2, rb, ra), BF16),
            pltpu.VMEM((na // 2, rb, ra), BF16),
            dma((nb,)), dma((nb,)), dma((na // 2,)), dma((na // 2,)), dma((na // 2,)), dma((na // 2,)), dma, dma,
            dma((nb, 2)), dma((nb, 2)), dma((na // 2,)), dma((na // 2,)), dma((na // 2,)), dma((na // 2,)),
        ],
        compiler_params=pltpu.CompilerParams(
            collective_id=0, has_side_effects=True, vmem_limit_bytes=56 * 1024 * 1024),
    )(amplitudes, code, counts.reshape(1, -1), pair_irrep.reshape(1, -1), integrals, one_body.reshape(1, -1))


def solution(mesh):
    placed = (P("aa", "ba"), P(), P(), P(), P(), P())
    body = functools.partial(per_device, mesh.shape["aa"], mesh.shape["ba"])
    return jax.shard_map(body, mesh=mesh, in_specs=placed, out_specs=P("aa", "ba"), check_vma=False)
```

```python
import functools

import jax
import jax.numpy as jnp
from jax import lax
from jax.experimental import pallas as pl
from jax.experimental.pallas import tpu as pltpu
from jax.sharding import PartitionSpec as P

F32 = jnp.float32
BF16 = jnp.bfloat16
MESH = pl.DeviceIdType.MESH
GATHER = 8
MIX = 16
LAG = 3


def iota(shape, axis):
    return lax.broadcasted_iota(jnp.int32, shape, axis)


def dot(a, b):
    return jnp.dot(a, b, preferred_element_type=F32)


def dot_nt(a, b):
    return lax.dot_general(a, b, (((1,), (1,)), ((), ())), preferred_element_type=F32)


def kernel(
    na, nb, capacity,
    amp_in, code_in, counts_in, irrep_in, integrals_in, one_body_in,
    out_ref,
    amp_ref, code_ref, counts_ref, irrep_ref, integrals_ref, one_body_ref, in_sem,
    hi_ref, lo_ref, sg_ref, kk_ref, m2_ref, mt_ref, y_ref, z_ref, zt_ref, kron_ref, live_ref,
    mg_ref, tb_ref, ta_ref, own_ref, xs_ref, xr_ref, rs_ref, rr_ref,
    m_send, m_recv, t_send, t_recv, f_send, f_recv, g_send, g_recv, c_send, c_recv, x_send, x_recv, r_send, r_recv,
):
    ra, rb = amp_ref.shape
    pairs, ns = code_ref.shape
    his = ns // 128
    half = his // 2
    tr = ns // (na * nb)
    keys = his * tr
    ma = lax.axis_index("aa")
    mb = lax.axis_index("ba")

    nc = na // 2
    chip = ma // 2
    core = lax.rem(ma, 2)
    sibling = chip * 2 + 1 - core

    nx = nc // 2
    ny = nb // 2
    z_hi = lax.rem(chip, 2)
    z_lo = lax.rem(mb, 2)

    def peer_chip(k):
        return lax.rem(chip + k, nc)

    def along_x(k, opposite):
        return lax.rem(chip // 2 + k, nx) * 2 + (1 - z_hi if opposite else z_hi)

    def along_y(k, opposite):
        return lax.rem(mb // 2 + k, ny) * 2 + (1 - z_lo if opposite else z_lo)

    def same_core(c):
        return c * 2 + core

    def peer_b(k):
        return lax.rem(mb + k, nb)

    barrier = pltpu.get_barrier_semaphore()
    for k in range(1, nb):
        pl.semaphore_signal(barrier, inc=1, device_id=(ma, peer_b(k)), device_id_type=MESH)
        pl.semaphore_signal(barrier, inc=1, device_id=(sibling, peer_b(k)), device_id_type=MESH)
    for k in range(1, nc):
        pl.semaphore_signal(barrier, inc=1, device_id=(same_core(peer_chip(k)), mb), device_id_type=MESH)
    pl.semaphore_signal(barrier, inc=1, device_id=(sibling, mb), device_id_type=MESH)
    loads = [
        pltpu.make_async_copy(src, dst, in_sem.at[i])
        for i, (src, dst) in enumerate((
            (amp_in, amp_ref), (code_in, code_ref), (counts_in, counts_ref), (irrep_in, irrep_ref),
            (integrals_in, integrals_ref), (one_body_in, one_body_ref)))
    ]
    for load in loads:
        load.start()
    loads[0].wait()
    pl.semaphore_wait(barrier, nc + 2 * (nb - 1))

    def m_copy(k, block, dest):
        return pltpu.make_async_remote_copy(
            src_ref=mg_ref.at[block], dst_ref=mg_ref.at[block], send_sem=m_send.at[k], recv_sem=m_recv.at[block],
            device_id=(ma, dest), device_id_type=MESH)

    def m_first(k):
        return pltpu.make_async_remote_copy(
            src_ref=amp_ref, dst_ref=mg_ref.at[mb], send_sem=m_send.at[k], recv_sem=m_recv.at[mb],
            device_id=(ma, along_y(k, k == 0)), device_id_type=MESH)

    def m_relay(k):
        return m_copy(ny + k, along_y(0, True), along_y(k, False))

    near = [k for k in range(1, ny) if k in (1, ny - 1)]
    far = [k for k in range(1, ny) if k not in near]
    for k in [0] + near + far:
        m_first(k).start()

    for load in loads[1:]:
        load.wait()

    code = code_ref[...]
    target = jnp.abs(code) - 1
    hi = lax.shift_right_arithmetic(target, 7)
    lo = target & 127
    sg = jnp.where(code > 0, 1.0, jnp.where(code < 0, -1.0, 0.0)).astype(F32)
    hi_ref[...] = hi.astype(F32)
    lo_ref[...] = lo.astype(F32)
    sg_ref[...] = sg

    blocks = counts_ref.shape[1]
    counts = jnp.broadcast_to(counts_ref[...].astype(F32), (8, blocks)).astype(BF16)
    spread = (iota((blocks, ns), 1) // capacity == iota((blocks, ns), 0)).astype(F32).astype(BF16)
    slots = (iota((8, ns), 1) % capacity).astype(F32)
    live8 = jnp.where(slots < dot(counts, spread), 1.0, 0.0)
    live = live8[0:1]
    live_ref[...] = live8

    irr = jnp.broadcast_to(irrep_ref[...], (pairs, pairs))
    eye = iota((pairs, pairs), 0) == iota((pairs, pairs), 1)
    irr_col = jnp.sum(jnp.where(eye, irr, 0), axis=1, keepdims=True)
    w = jnp.where(irr_col == irr, integrals_ref[...].astype(F32), 0.0).astype(BF16)
    w_t = dot_nt(eye.astype(F32).astype(BF16), w).astype(BF16)

    first = mb * rb + ma * tr
    base = pl.multiple_of((first // 128) * 128, 128)
    off = first - base
    n = pairs * tr
    own = jnp.concatenate(
        [hi_ref[:, pl.ds(base, 128)], lo_ref[:, pl.ds(base, 128)], sg_ref[:, pl.ds(base, 128)]], axis=0
    ).astype(BF16)
    pick = (iota((128, n), 0) == off + iota((128, n), 1) % tr).astype(F32).astype(BF16)
    mine = dot(own, pick)
    here = iota((pairs, n), 0) == iota((pairs, n), 1) // tr
    k_hi = jnp.sum(jnp.where(here, mine[0:pairs], 0.0), axis=0, keepdims=True)
    k_lo = jnp.sum(jnp.where(here, mine[pairs : 2 * pairs], 0.0), axis=0, keepdims=True)
    k_sg = jnp.sum(jnp.where(here, mine[2 * pairs :], 0.0), axis=0, keepdims=True)
    here_b = here.astype(F32).astype(BF16)
    w_wide = dot(w_t, here_b)
    o_wide = dot(jnp.broadcast_to(one_body_ref[...], (8, pairs)), here_b)[0:1]
    k_lo_b = k_lo.astype(BF16)
    iota128 = iota((128, n), 0).astype(F32).astype(BF16)
    one = jnp.ones((), BF16)
    zero = jnp.zeros((), BF16)
    planes = jnp.concatenate([hi_ref[...], lo_ref[...], sg_ref[...] * live], axis=0).astype(BF16)
    got = jnp.zeros((3 * pairs, n), F32)
    for h in range(0, his, 2):
        sel = []
        for e in range(2):
            loc = jnp.where(k_hi == float(h + e), k_lo, -1.0).astype(BF16)
            sel.append(jnp.where(iota128 == loc, one, zero))
        got = got + dot(planes[:, h * 128 : (h + 2) * 128], jnp.concatenate(sel, axis=0))
    row = (iota((pairs, n), 1) % tr).astype(F32)

    def split(high, low):
        upper = jnp.floor(high * 0.5)
        return upper * float(tr), (high - 2.0 * upper) * 128.0 + low

    key_all, low_all = split(got[0:pairs], got[pairs : 2 * pairs])
    key_all = (key_all + row).astype(BF16)
    val_all = (0.5 * w_wide * got[2 * pairs :] * k_sg).astype(BF16)
    key_one, low_one = split(k_hi, k_lo)
    key_one = (key_one + row[0:1]).astype(BF16)
    low_t = jnp.concatenate([low_all, jnp.broadcast_to(low_one, (8, n))], axis=0).T
    low_t = low_t.astype(BF16)
    iota_keys = iota((keys // 2, n), 0).astype(F32).astype(BF16)
    iota_low = iota((n, 256), 1).astype(F32).astype(BF16)

    def histogram(key, val, at):
        a = jnp.where(iota_keys == key, val, zero)
        hit = iota_low == jnp.broadcast_to(low_t[:, at : at + 1], (n, 256))
        b = jnp.where(hit, one, zero)
        return dot(a, b)

    t_acc = histogram(key_one, (o_wide * k_sg).astype(BF16), pairs)
    for q in range(pairs):
        t_acc = t_acc + histogram(key_all[q : q + 1], val_all[q : q + 1], q)
    t_acc = t_acc.astype(BF16)
    for h in range(2):
        part = t_acc[:, h * 128 : (h + 1) * 128].reshape(his // 2, tr, 128)
        for g in range(his // 2):
            tb_ref[ma, 2 * g + h] = part[g]

    def t_copy(k, c, dest):
        slot = same_core(c)
        return pltpu.make_async_remote_copy(
            src_ref=tb_ref.at[slot], dst_ref=tb_ref.at[slot], send_sem=t_send.at[k], recv_sem=t_recv.at[c],
            device_id=(same_core(dest), mb), device_id_type=MESH)

    def t_first(k):
        return t_copy(k, chip, along_x(k, k == 0))

    def t_relay(k):
        return t_copy(nx + k, along_x(0, True), along_x(k, False))

    def f_copy(c):
        slot = same_core(c)
        return pltpu.make_async_remote_copy(
            src_ref=tb_ref.at[slot], dst_ref=tb_ref.at[slot], send_sem=f_send.at[c], recv_sem=f_recv.at[c],
            device_id=(sibling, mb), device_id_type=MESH)

    def f_arrived(c):
        slot = c * 2 + 1 - core
        return pltpu.make_async_remote_copy(
            src_ref=tb_ref.at[slot], dst_ref=tb_ref.at[slot], send_sem=f_send.at[c], recv_sem=f_recv.at[c],
            device_id=(sibling, mb), device_id_type=MESH)

    hc = nc // 2
    lag = min(LAG, hc)

    def pass_on(c):
        for k in range(1, nb):
            pltpu.make_async_remote_copy(
                src_ref=tb_ref.at[same_core(c), pl.ds(chip * 2, 2)], dst_ref=ta_ref.at[mb, core, lax.rem(c, hc)],
                send_sem=c_send.at[k, c // hc], recv_sem=c_recv.at[mb, core],
                device_id=(chip * 2 + c // hc, peer_b(k)), device_id_type=MESH).start()

    def c_copy(k, src, e):
        return pltpu.make_async_remote_copy(
            src_ref=ta_ref.at[src, e], dst_ref=ta_ref.at[src, e], send_sem=c_send.at[k, e],
            recv_sem=c_recv.at[src, e], device_id=(chip * 2 + e, peer_b(k)), device_id_type=MESH)

    def hand_over(c):
        t_copy(0, c, chip).wait_recv()
        f_copy(c).start()
        pass_on(c)

    near_x = [k for k in range(1, nx) if k in (1, nx - 1)]
    far_x = [k for k in range(1, nx) if k not in near_x]
    for k in [0] + near_x + far_x:
        t_first(k).start()
    f_copy(chip).start()
    pass_on(chip)

    m_copy(0, along_y(0, True), mb).wait_recv()
    for k in near + far:
        m_relay(k).start()

    grow = (iota((pairs * 8, pairs), 0) // 8 == iota((pairs * 8, pairs), 1)).astype(F32).astype(BF16)
    wide = dot_nt(dot(grow, w).astype(BF16), grow)
    same = iota((pairs * 8, pairs * 8), 0) % 8 == iota((pairs * 8, pairs * 8), 1) % 8
    kron_ref[...] = jnp.where(same, wide, 0.0).astype(BF16)

    low_a = ma * ra
    block_of = (iota((ra, blocks), 0) + low_a) // capacity
    count_a = jnp.sum(
        jnp.where(block_of == iota((ra, blocks), 1), counts_ref[...].astype(F32), 0.0), axis=1, keepdims=True)
    live_a = jnp.where(((iota((ra, 1), 0) + low_a) % capacity).astype(F32) < count_a, 1.0, 0.0)
    mg_ref[mb] = amp_ref[...]
    low_b = pl.multiple_of(mb * rb, 128)
    live_b = live_ref[0:1, pl.ds(low_b, rb)]
    mine_f = amp_ref[...].astype(F32) * live_a * live_b
    mt_ref[core] = mine_f.T.astype(BF16)
    g_copy = pltpu.make_async_remote_copy(
        src_ref=mt_ref.at[core], dst_ref=mt_ref.at[core], send_sem=g_send, recv_sem=g_recv,
        device_id=(sibling, mb), device_id_type=MESH)
    g_copy.start()

    hi_b = hi_ref[:, pl.ds(low_b, rb)]
    y_b = jnp.floor(hi_b * 0.25)
    rest_b = hi_b - 4.0 * y_b
    for turn in range(2):
        e_b = rest_b - 2.0 * (1 - z_lo if turn else z_lo).astype(F32)
        inside = (e_b >= 0.0) & (e_b < 2.0)
        kk_ref[turn] = jnp.where(inside, 2.0 * y_b + e_b, -1.0)

    iota_b = iota((128, rb), 0).astype(F32).astype(BF16)

    def arrange(turn):
        for y in range(ny):
            block = 2 * y + (1 - z_lo if turn else z_lo)
            on = live_ref[0:1, pl.ds(pl.multiple_of(block * rb, 128), rb)]
            part = (mg_ref[block].astype(F32) * live_a * on).astype(BF16)
            for e in range(2):
                u = 2 * y + e
                h, at = u // ny, (u % ny) * 128
                m2_ref[turn, h * ra : (h + 1) * ra, at : at + 128] = part[:, e * 128 : (e + 1) * 128]

    def gather_one(turn, q):
        kk_q = kk_ref[turn, pl.ds(q, 1), :]
        lo_q = lo_ref[pl.ds(q, 1), pl.ds(low_b, rb)]
        sg_q = sg_ref[pl.ds(q, 1), pl.ds(low_b, rb)]
        upper = kk_q >= float(ny)
        inner = jnp.where(upper, kk_q - float(ny), kk_q)
        hots = []
        for j in range(ny):
            loc = jnp.where(inner == float(j), lo_q, -1.0).astype(BF16)
            hots.append(jnp.where(iota_b == loc, one, zero))
        got_q = dot(m2_ref[turn], jnp.concatenate(hots, axis=0))
        picked = jnp.where(jnp.broadcast_to(upper, (ra, rb)), got_q[ra:], got_q[:ra]) * (sg_q * live_b)
        if turn:
            z_ref[q] = (y_ref[q] + picked).astype(BF16).T.astype(F32)
        else:
            y_ref[q] = picked

    trips = pairs // GATHER

    for k in range(1, ny):
        m_copy(0, along_y(k, False), mb).wait_recv()
    arrange(0)

    def gather_own(i, carry):
        for e in range(GATHER):
            gather_one(0, i * GATHER + e)

        @pl.when(i == trips - 3)
        def _():
            t_copy(0, along_x(0, True), chip).wait_recv()
            for k in near_x + far_x:
                t_relay(k).start()
            f_copy(along_x(0, True)).start()
            pass_on(along_x(0, True))
        return carry

    lax.fori_loop(0, trips, gather_own, 0)
    for k in near_x + far_x:
        hand_over(along_x(k, False))
    for k in range(1, ny):
        m_copy(0, along_y(k, True), mb).wait_recv()
    arrange(1)

    def gather_other(i, carry):
        for e in range(GATHER):
            gather_one(1, i * GATHER + e)

        @pl.when(i == trips - 2)
        def _():
            for k in near_x:
                hand_over(along_x(k, True))
        return carry

    lax.fori_loop(0, trips, gather_other, 0)
    for k in far_x:
        hand_over(along_x(k, True))

    def mix(i, carry):
        for e in range(MIX):
            at = pl.multiple_of((i * MIX + e) * 16, 16)
            rows = [z_ref[:, pl.ds(at + 8 * h, 8), :].reshape(pairs * 8, ra) for h in range(2)]
            mixed = dot(kron_ref[...], jnp.concatenate(rows, axis=1).astype(BF16)).reshape(pairs, 8, 2 * ra)
            zt_ref[:, pl.ds(at, 16), :] = jnp.concatenate([mixed[:, :, :ra], mixed[:, :, ra:]], axis=1).astype(BF16)
        return carry

    lax.fori_loop(0, rb // 16 // MIX, mix, 0)


    width = 2 * ra
    group = min(pairs, 4)

    def x_copy(c):
        return pltpu.make_async_remote_copy(
            src_ref=xs_ref.at[c], dst_ref=xr_ref.at[c], send_sem=x_send.at[c], recv_sem=x_recv.at[c],
            device_id=(sibling, mb), device_id_type=MESH)

    def r_copy(c):
        return pltpu.make_async_remote_copy(
            src_ref=rs_ref.at[c], dst_ref=rr_ref.at[chip], send_sem=r_send.at[c], recv_sem=r_recv.at[chip],
            device_id=(same_core(c), mb), device_id_type=MESH)

    def r_arrived(c):
        return pltpu.make_async_remote_copy(
            src_ref=rs_ref.at[c], dst_ref=rr_ref.at[c], send_sem=r_send.at[c], recv_sem=r_recv.at[c],
            device_id=(same_core(c), mb), device_id_type=MESH)

    def scatter(i, carry):
        d = turn_of(i)
        at = pl.multiple_of(d * width, 128)
        acc = jnp.zeros((rb, width), F32)
        for p0 in range(0, pairs, group):
            hots = []
            for p in range(p0, p0 + group):
                hit = hi_ref[p : p + 1, pl.ds(at, width)] == ma.astype(F32)
                loc = jnp.where(hit, lo_ref[p : p + 1, pl.ds(at, width)], -1.0).astype(BF16)
                hots.append(jnp.where(iota_b == loc, sg_ref[p : p + 1, pl.ds(at, width)].astype(BF16), zero))
            lhs = jnp.concatenate([zt_ref[p] for p in range(p0, p0 + group)], axis=1)
            acc = acc + dot(lhs, jnp.concatenate(hots, axis=0))
        first_core = core == 0
        own_ref[d] = jnp.where(first_core, acc[:, :ra], acc[:, ra:])
        xs_ref[d] = jnp.where(first_core, acc[:, ra:], acc[:, :ra])
        x_copy(d).start()

        @pl.when(i == lag - 1)
        def _():
            for c in range(nc):
                f_arrived(c).wait_recv()
            for e in range(2):
                for c in range(hc):
                    ta_ref[mb, e, c] = tb_ref[core * nc + 2 * c + e, pl.ds(chip * 2, 2)]
            g_copy.wait()

        @pl.when(i >= lag)
        def _():
            send(turn_of(i - lag))

        @pl.when(i == nc - 1)
        def _():
            if lag > 1:
                send(turn_of(nc - lag))
        return carry

    def turn_of(i):
        return lax.rem(chip // 2 + nx - 1 - lax.rem(i, nx), nx) * 2 + jnp.where(i < nx, 1 - z_hi, z_hi)

    def arrival(i):
        return lax.rem(chip // 2 + 1 + i % nx, nx) * 2 + (1 - z_hi if i < nx else z_hi)

    def summed(d):
        @pl.when(d != mb)
        def _():
            for e in range(2):
                c_copy(1, d, e).wait_recv()
        x_copy(d).wait_recv()
        acc = own_ref[d] + xr_ref[d]
        for h in range(2):
            rows = jnp.concatenate([ta_ref[d, e, c, h] for c in range(hc) for e in range(2)], axis=0)
            acc = acc + dot_nt(mt_ref[h], rows)
        return acc

    def send(d):
        rs_ref[d] = summed(d).astype(BF16)
        r_copy(d).start()

    lax.fori_loop(0, nc, scatter, 0)
    for i in range(nc - lag + 1, nc - 1):
        send(turn_of(i))

    res = jnp.zeros((rb, ra), F32)
    for turn in range(2):
        for u in range(0, 2 * ny, min(ny, 2)):
            parts = []
            for v in range(u, u + min(ny, 2)):
                h = 4 * (v // 2) + 2 * (1 - z_lo if turn else z_lo) + v % 2
                parts.append(tb_ref[:, h].reshape(rb, 128))
            h, at = u // ny, (u % ny) * 128
            res = res + dot_nt(
                jnp.concatenate(parts, axis=1), m2_ref[turn, h * ra : (h + 1) * ra, at : at + 128 * len(parts)])


    out_t = res + summed(chip)
    for i in range(nc - 1):
        c = arrival(i)
        r_arrived(c).wait_recv()
        out_t = out_t + rr_ref[c].astype(F32)
    out_ref[...] = (out_t.T * live_a * live_b).astype(BF16)

    for k in range(ny):
        m_first(k).wait_send()
    for k in range(1, ny):
        m_relay(k).wait_send()
    for k in range(nx):
        t_first(k).wait_send()
    for k in range(1, nx):
        t_relay(k).wait_send()
    for k in range(1, nb):
        for e in range(2):
            c_copy(k, mb, e).wait_send()
    for c in range(nc):
        f_copy(c).wait_send()
        x_copy(c).wait_send()
    for k in range(1, nc):
        r_copy(peer_chip(k)).wait_send()


def per_device(na, nb, amplitudes, code, counts, pair_irrep, integrals, one_body):
    ra, rb = amplitudes.shape
    pairs, ns = code.shape
    his = ns // 128
    tr = ns // (na * nb)
    dma = pltpu.SemaphoreType.DMA
    vmem = pl.BlockSpec(memory_space=pltpu.VMEM)
    return pl.pallas_call(
        functools.partial(kernel, na, nb, ns // counts.shape[0]),
        out_shape=jax.ShapeDtypeStruct((ra, rb), BF16),
        in_specs=[pl.BlockSpec(memory_space=pl.ANY)] * 6,
        out_specs=vmem,
        scratch_shapes=[
            pltpu.VMEM((ra, rb), BF16),
            pltpu.VMEM((pairs, ns), jnp.int32),
            pltpu.VMEM((1, counts.shape[0]), jnp.int32),
            pltpu.VMEM((1, pairs), jnp.int32),
            pltpu.VMEM((pairs, pairs), BF16),
            pltpu.VMEM((1, pairs), BF16),
            dma((6,)),
            pltpu.VMEM((pairs, ns), F32),
            pltpu.VMEM((pairs, ns), F32),
            pltpu.VMEM((pairs, ns), F32),
            pltpu.VMEM((2, pairs, rb), F32),
            pltpu.VMEM((2, 2 * ra, ns // 4), BF16),
            pltpu.VMEM((2, rb, ra), BF16),
            pltpu.VMEM((pairs, ra, rb), F32),
            pltpu.VMEM((pairs, rb, ra), F32),
            pltpu.VMEM((pairs, rb, ra), BF16),
            pltpu.VMEM((pairs * 8, pairs * 8), BF16),
            pltpu.VMEM((8, ns), F32),
            pltpu.VMEM((nb, ra, rb), BF16),
            pltpu.VMEM((na, his, tr, 128), BF16),
            pltpu.VMEM((nb, 2, na // 4, 2, tr, 128), BF16),
            pltpu.VMEM((na // 2, rb, ra), F32),
            pltpu.VMEM((na // 2, rb, ra), F32),
            pltpu.VMEM((na // 2, rb, ra), F32),
            pltpu.VMEM((na // 2, rb, ra), BF16),
            pltpu.VMEM((na // 2, rb, ra), BF16),
            dma((nb,)), dma((nb,)), dma((na // 2,)), dma((na // 2,)), dma((na // 2,)), dma((na // 2,)), dma, dma,
            dma((nb, 2)), dma((nb, 2)), dma((na // 2,)), dma((na // 2,)), dma((na // 2,)), dma((na // 2,)),
        ],
        compiler_params=pltpu.CompilerParams(
            collective_id=0, has_side_effects=True, vmem_limit_bytes=56 * 1024 * 1024),
    )(amplitudes, code, counts.reshape(1, -1), pair_irrep.reshape(1, -1), integrals, one_body.reshape(1, -1))


def solution(mesh):
    placed = (P("aa", "ba"), P(), P(), P(), P(), P())
    body = functools.partial(per_device, mesh.shape["aa"], mesh.shape["ba"])
    return jax.shard_map(body, mesh=mesh, in_specs=placed, out_specs=P("aa", "ba"), check_vma=False)
```
